256 devices in a mesh: groups: 2 (over y), row: 32 (over z, core), col: 4 (over x).
Axes of the slice: x: 4, y: 2, z: 16, core: 2. Of those that a mesh axis runs over, the one named last changes fastest.
The devices are a block of a 4x16x16 slice.
Arguments:
- pair_grid: bfloat16 [1024, 512, 128], P(('groups', 'row'), 'col'), parts along dimension 0, may hold values from -6 to 6
- alignment_pool: bfloat16 [512, 512, 64], P('groups', 'row'), parts along dimension 0, may hold values from -6 to 6
- sample_index: int32 [128], P('groups'), parts along dimension 0, may hold values from 0 to 255
- token_mask: int32 [1024], P('groups'), parts along dimension 0, may hold values 0 or 1
- outer_proj: bfloat16 [64, 64], replicated, may hold values from -0.75 to 0.75
- outer_mix: bfloat16 [1024, 128], replicated, may hold values from -0.375 to 0.375
- pair_logit: bfloat16 [128, 8], replicated, may hold values from -1 to 1
- average_proj: bfloat16 [64, 512], replicated, may hold values from -0.75 to 0.75
- average_mix: bfloat16 [256, 64], replicated, may hold values from -0.75 to 0.75
- triangle_proj: bfloat16 [128, 640], replicated, may hold values from -0.5 to 0.5
- triangle_mix: bfloat16 [128, 128], replicated, may hold values from -0.5 to 0.5
- transition_up: bfloat16 [128, 1024], replicated, may hold values from -0.5 to 0.5
- transition_down: bfloat16 [512, 128], replicated, may hold values from -0.25 to 0.25
Outputs:
- pair_next: bfloat16 [1024, 512, 128], P(('groups', 'row'), 'col'), parts along dimension 0
- alignment_next: bfloat16 [128, 512, 64], P('groups', 'row'), parts along dimension 0
The draws below stay inside these ranges and needn't reach their ends.
There are 2 independent parts, one for each index of `groups`. The reference program is written for one: setup_inputs(seed, part) draws one part's arguments, and reference() takes and returns one part's arrays. A program takes and returns all parts, laid end to end along the dimension named above; an argument that names none is the same for every part. Nothing has to cross between parts.
Inputs may be any that keep to these rules, and one draw needn't show every extreme that they name: `sample_index`: indices into the first dimension of alignment_pool; they may repeat. `token_mask`: 1 marks a real residue, 0 a padded one.
All inputs are finite; a program needn't handle non-finite values.
Results may differ from the reference program's by a relative error of at most 0.008.
Values may be sent and summed in bfloat16 or wider, within the bound.
No kernel may reach another device: no remote copies, remote signals or barrier semaphores. Data moves between devices by JAX's collectives and lax.ppermute only.
A program may use at most 64 MiB of HBM per device.

```python
import math
import jax
import jax.numpy as jnp
from jax import lax

C = 128
CM = 64
OPC = 32
H = 8
HC = 32
TR = 512
S = 64
POOL = 256
N = 512


def with_ends(drawn, stream_key, least, top_value):
    spot = [jax.random.randint(jax.random.fold_in(stream_key, axis), (), 0, length) for axis, length in enumerate(drawn.shape)]
    main_axis = drawn.shape.index(max(drawn.shape))
    beside = spot[:main_axis] + [(spot[main_axis] + 1) % drawn.shape[main_axis]] + spot[main_axis + 1:]
    return drawn.at[tuple(spot)].set(least).at[tuple(beside)].set(top_value)


def steps_of(rng, dims, pieces, low, largest):
    level, own = 1.0, jax.random.fold_in(rng, 6)
    for axis_at, shards_of in pieces:
        heights = jnp.exp(jax.random.uniform(jax.random.fold_in(own, axis_at), (shards_of,), jnp.float32, low / len(pieces), largest / len(pieces)))
        level = level * jnp.repeat(heights, dims[axis_at] // shards_of).reshape([-1 if axis == axis_at else 1 for axis in range(len(dims))])
    return level


def normal_values(stream_key, extent, scale, bound, shards=(), kind=jnp.bfloat16):
    gain = steps_of(stream_key, extent, shards, -0.22, 0.18) if shards else 1.0
    array = jax.random.normal(stream_key, extent, jnp.float32) * scale * gain
    return jnp.minimum(jnp.maximum(array, -bound), bound).astype(kind)


def setup_inputs(seed: int = 0, part: int = 0) -> dict:
    splits = jax.random.split(jax.random.key(seed), 14)
    part_keys = jax.random.split(jax.random.fold_in(splits[13], part), 14)
    pair_grid = normal_values(part_keys[0], (N, N, C), 1.0, 6.0, ((0, 32), (1, 4)))
    alignment_pool = normal_values(part_keys[1], (POOL, N, CM), 1.0, 6.0, ((1, 32),))
    sample_index = with_ends(jax.random.randint(part_keys[2], (S,), 0, POOL), jax.random.fold_in(part_keys[2], 1), 0, POOL - 1).astype(jnp.int32)
    token_mask = with_ends((jax.random.randint(part_keys[3], (N,), 0, 8) < 7).astype(jnp.int32), jax.random.fold_in(part_keys[3], 1), 0, 1)
    outer_proj = normal_values(splits[4], (CM, 2 * OPC), CM ** -0.5, 0.75)
    outer_mix = normal_values(splits[5], (OPC * OPC, C), (OPC * OPC // 4) ** -0.5, 0.375)
    pair_logit = normal_values(splits[6], (C, H), (C // 4) ** -0.5, 1.0)
    average_proj = normal_values(splits[7], (CM, 2 * H * HC), CM ** -0.5, 0.75)
    average_mix = normal_values(splits[8], (H * HC, CM), (H * HC // 4) ** -0.5, 0.75)
    triangle_proj = normal_values(splits[9], (C, 5 * C), C ** -0.5, 0.5)
    triangle_mix = normal_values(splits[10], (C, C), C ** -0.5, 0.5)
    transition_up = normal_values(splits[11], (C, 2 * TR), C ** -0.5, 0.5)
    transition_down = normal_values(splits[12], (TR, C), TR ** -0.5, 0.25)
    return dict(pair_grid=pair_grid, alignment_pool=alignment_pool, sample_index=sample_index, token_mask=token_mask, outer_proj=outer_proj, outer_mix=outer_mix, pair_logit=pair_logit, average_proj=average_proj, average_mix=average_mix, triangle_proj=triangle_proj, triangle_mix=triangle_mix, transition_up=transition_up, transition_down=transition_down)


epsilon = 1e-05

def normalize(values, channel_dim):
    values = values.astype(jnp.float32)
    centred = values - lax.optimization_barrier(jnp.mean(values, axis=channel_dim, keepdims=True))
    spread = lax.optimization_barrier(jnp.mean(centred * centred, axis=channel_dim, keepdims=True))
    return centred / jnp.sqrt(spread + epsilon)

def settle_wide(values):
    return lax.optimization_barrier(values).astype(jnp.float32)

def reference(pair_grid, alignment_pool, sample_index, token_mask, outer_proj, outer_mix, pair_logit, average_proj, average_mix, triangle_proj, triangle_mix, transition_up, transition_down):
    alignments = jnp.take(alignment_pool, sample_index, axis=0)
    align_norm = normalize(alignments, 2).astype(jnp.bfloat16)
    align_flat = align_norm.reshape(S * N, CM)
    row_factor = jnp.dot(align_flat, outer_proj[:, :OPC], preferred_element_type=jnp.float32).astype(jnp.bfloat16).reshape(S, N, OPC)
    column_factor = jnp.dot(align_flat, outer_proj[:, OPC:], preferred_element_type=jnp.float32).astype(jnp.bfloat16).reshape(S, N, OPC)
    column_wide = settle_wide(column_factor)
    block_rows = math.gcd(N, 32)
    start_rows = (jnp.arange(N // block_rows) * block_rows).astype(jnp.int32)

    def outer_step(first_row):
        left_block = settle_wide(lax.dynamic_slice_in_dim(row_factor, first_row, block_rows, 1))
        outer_sum = jnp.einsum('sic,sjd->ijcd', left_block, column_wide)
        outer_mean = (outer_sum * (1.0 / S)).astype(jnp.bfloat16).reshape(block_rows * N, OPC * OPC)
        pair_update = jnp.dot(outer_mean, outer_mix, preferred_element_type=jnp.float32).reshape(block_rows, N, C)
        pair_block = lax.dynamic_slice_in_dim(pair_grid, first_row, block_rows, 0)
        return (pair_block.astype(jnp.float32) + pair_update).astype(jnp.bfloat16)
    pair_one = lax.map(outer_step, start_rows).reshape(N, N, C)
    pair_norm = normalize(pair_one, 2).astype(jnp.bfloat16)
    flat_norm = pair_norm.reshape(N * N, C)
    scores = jnp.dot(flat_norm, pair_logit, preferred_element_type=jnp.float32).reshape(N, N, H)
    weights = jnp.exp(scores)
    totals = lax.optimization_barrier(jnp.sum(weights, axis=1))
    column_values = jnp.dot(align_flat, average_proj[:, :H * HC], preferred_element_type=jnp.float32).astype(jnp.bfloat16).reshape(S, N, H, HC)
    gate_values = jax.nn.sigmoid(jnp.dot(align_flat, average_proj[:, H * HC:], preferred_element_type=jnp.float32)).reshape(S, N, H, HC)
    weighted = jnp.einsum('ijh,sjhc->sihc', settle_wide(weights.astype(jnp.bfloat16)), settle_wide(column_values))
    averaged = (gate_values * weighted / totals[None, :, :, None]).astype(jnp.bfloat16).reshape(S * N, H * HC)
    align_update = jnp.dot(averaged, average_mix, preferred_element_type=jnp.float32).reshape(S, N, CM)
    alignment_next = (alignments.astype(jnp.float32) + align_update).astype(jnp.bfloat16)
    mask_values = token_mask.astype(jnp.float32)
    pair_mask = mask_values[:, None] * mask_values[None, :]

    def channel_step(channel):
        picks = channel + C * jnp.arange(4, dtype=jnp.int32)
        columns = jnp.take(triangle_proj, picks, axis=1)
        projected = jnp.dot(flat_norm, columns, preferred_element_type=jnp.float32).reshape(N, N, 4)
        left_side = (jax.nn.sigmoid(projected[:, :, 0]) * projected[:, :, 1] * pair_mask).astype(jnp.bfloat16)
        right_side = (jax.nn.sigmoid(projected[:, :, 2]) * projected[:, :, 3] * pair_mask).astype(jnp.bfloat16)
        return jnp.dot(left_side, right_side.T, preferred_element_type=jnp.float32).astype(jnp.bfloat16)
    product = lax.map(channel_step, jnp.arange(C, dtype=jnp.int32))
    gate_weight = triangle_proj[:, 4 * C:]
    pair_rows_all = pair_one.reshape(N * N, C)

    def tail_step(first_row):
        product_block = lax.dynamic_slice_in_dim(product, first_row, block_rows, 1)
        product_norm = normalize(product_block, 0).astype(jnp.bfloat16).reshape(C, block_rows * N)
        mixed = lax.dot_general(product_norm, triangle_mix, (((0,), (0,)), ((), ())), preferred_element_type=jnp.float32)
        norm_rows = lax.dynamic_slice_in_dim(flat_norm, first_row * N, block_rows * N, 0)
        gate_out = jax.nn.sigmoid(jnp.dot(norm_rows, gate_weight, preferred_element_type=jnp.float32))
        pair_rows = lax.dynamic_slice_in_dim(pair_rows_all, first_row * N, block_rows * N, 0)
        pair_two = (pair_rows.astype(jnp.float32) + gate_out * mixed).astype(jnp.bfloat16)
        normed = normalize(pair_two, 1).astype(jnp.bfloat16)
        expanded = jnp.dot(normed, transition_up, preferred_element_type=jnp.float32)
        hidden = (jax.nn.silu(expanded[:, :TR]) * expanded[:, TR:]).astype(jnp.bfloat16)
        return (settle_wide(pair_two) + jnp.dot(hidden, transition_down, preferred_element_type=jnp.float32)).astype(jnp.bfloat16)
    pair_next = lax.map(tail_step, start_rows).reshape(N, N, C)
    return (pair_next, alignment_next)
```

```python
import functools

import jax
import jax.numpy as jnp
from jax import lax
from jax.experimental import pallas as pl
from jax.experimental.pallas import tpu as pltpu
from jax.sharding import Mesh
from jax.sharding import PartitionSpec as P

ROW = ("part", "near", "core")
ROW_COL = ("part", "near", "core", "col")
GROUPS_ROW = ("groups", "part", "near", "core")

epsilon = 1e-05
f32 = jnp.float32
bf16 = jnp.bfloat16
NT = (((1,), (1,)), ((), ()))
TN = (((0,), (0,)), ((), ()))


def normalize(values, channel_dim):
    values = values.astype(f32)
    centred = values - jnp.mean(values, axis=channel_dim, keepdims=True)
    spread = jnp.mean(centred * centred, axis=channel_dim, keepdims=True)
    return centred * lax.rsqrt(spread + epsilon)


def sigmoid(x):
    return 1.0 / (1.0 + jnp.exp(-x))


def whole(shape):
    return pl.BlockSpec(shape, lambda *_: (0,) * len(shape))


def mix_kernel(norm_ref, proj_ref, mix_ref, out_ref, rows_ref, *, scale, group):
    width = mix_ref.shape[2]
    tokens = norm_ref.shape[0]
    samples = norm_ref.shape[1]

    @pl.when(pl.program_id(0) == 0)
    def _():
        flat = norm_ref[...].reshape(tokens * samples, norm_ref.shape[2])
        rows_ref[...] = jnp.dot(flat, proj_ref[...], preferred_element_type=f32).astype(bf16)

    both = jnp.concatenate([mix_ref[0], mix_ref[1]], axis=1)
    part = jnp.dot(rows_ref[...], both, preferred_element_type=f32) * scale
    part = part.astype(bf16)
    for d in range(2):
        for i in range(tokens):
            for g in range(samples // group):
                out_ref[g, d, :, i * width : (i + 1) * width] = part[
                    i * samples + g * group : i * samples + (g + 1) * group,
                    d * width : (d + 1) * width,
                ]


def mixed_rows(norm_t, proj, mix_d, group):
    tokens, samples, _ = norm_t.shape
    depth, inner, width = mix_d.shape
    groups = samples // group
    out = pl.pallas_call(
        functools.partial(mix_kernel, scale=1.0 / samples, group=group),
        grid=(depth // 2,),
        in_specs=[
            whole(norm_t.shape),
            whole(proj.shape),
            pl.BlockSpec((2, inner, width), lambda d: (d, 0, 0)),
        ],
        out_specs=pl.BlockSpec((groups, 2, group, tokens * width), lambda d: (0, d, 0, 0)),
        out_shape=jax.ShapeDtypeStruct((groups, depth, group, tokens * width), bf16),
        scratch_shapes=[pltpu.VMEM((tokens * samples, inner), bf16)],
        cost_estimate=pl.CostEstimate(
            flops=16 * tokens * samples * inner * depth * width,
            bytes_accessed=2 * tokens * samples * depth * width,
            transcendentals=0,
        ),
        name="mixed_rows",
    )(norm_t, proj, mix_d)
    return out.reshape(groups * depth * group, tokens * width)


def pair_kernel(
    norm_ref, spread_ref, mixed_ref, pair_ref, proj_ref, logit_ref, mask_ref,
    one_ref, pnorm_ref, weight_ref, factor_ref, col_ref, left_ref, right_ref,
):
    step = pl.program_id(0)
    cols, width = pair_ref.shape[1], pair_ref.shape[2]
    tokens = factor_ref.shape[2]
    chunk, got = spread_ref.shape

    @pl.when(step == 0)
    def _():
        for g in range(norm_ref.shape[1] // chunk):
            col_ref[:, g * got : (g + 1) * got] = jnp.dot(
                norm_ref[:, g * chunk : (g + 1) * chunk], spread_ref[...],
                preferred_element_type=f32,
            ).astype(bf16)

    update = jnp.dot(col_ref[...], mixed_ref[...], preferred_element_type=f32)
    normed = []
    for n in range(2):
        one = (pair_ref[n].astype(f32) + update[:, n * width : (n + 1) * width]).astype(bf16)
        one_ref[n] = one
        now = normalize(one, 1).astype(bf16)
        pnorm_ref[n] = now
        normed.append(now)
    normed = jnp.concatenate(normed, axis=0)
    projected = lax.dot_general(proj_ref[...], normed, NT, preferred_element_type=f32)
    scores = jnp.exp(lax.dot_general(logit_ref[...], normed, NT, preferred_element_type=f32))
    left = sigmoid(projected[:width]) * projected[width : 2 * width]
    right = sigmoid(projected[2 * width : 3 * width]) * projected[3 * width :]
    for n in range(2):
        weight_ref[n] = scores[:, n * cols : (n + 1) * cols]
        mask = mask_ref[n]
        lanes = slice(n * cols, (n + 1) * cols)
        at = pl.ds(step * 2 + n, width, stride=tokens)
        left_ref[at, :] = left[:, lanes] * mask
        right_ref[at, :] = right[:, lanes] * mask

    @pl.when(step == pl.num_programs(0) - 1)
    def _():
        factor_ref[:, 0] = left_ref[...].reshape(width, tokens, cols).astype(bf16)
        factor_ref[:, 1] = right_ref[...].reshape(width, tokens, cols).astype(bf16)


def pair_part(norm_rows, spread, mixed, pair_grid, proj_t, logit_t, mask):
    tokens, cols, width = pair_grid.shape
    heads = logit_t.shape[0]
    depth = mixed.shape[0]
    pairs = pl.BlockSpec((2, cols, width), lambda n: (n, 0, 0))
    return pl.pallas_call(
        pair_kernel,
        grid=(tokens // 2,),
        in_specs=[
            whole(norm_rows.shape),
            whole(spread.shape),
            pl.BlockSpec((depth, 2 * width), lambda n: (0, n)),
            pairs,
            whole(proj_t.shape),
            whole(logit_t.shape),
            pl.BlockSpec((2, 1, cols), lambda n: (n, 0, 0)),
        ],
        out_specs=[
            pairs,
            pairs,
            pl.BlockSpec((2, heads, cols), lambda n: (n, 0, 0)),
            whole((width, 2, tokens, cols)),
        ],
        out_shape=[
            jax.ShapeDtypeStruct(pair_grid.shape, bf16),
            jax.ShapeDtypeStruct(pair_grid.shape, bf16),
            jax.ShapeDtypeStruct((tokens, heads, cols), f32),
            jax.ShapeDtypeStruct((width, 2, tokens, cols), bf16),
        ],
        scratch_shapes=[
            pltpu.VMEM((cols, depth), bf16),
            pltpu.VMEM((width * tokens, cols), f32),
            pltpu.VMEM((width * tokens, cols), f32),
        ],
        name="pair_part",
    )(norm_rows, spread, mixed, pair_grid, proj_t, logit_t, mask)


def triangle_kernel(got_ref, out_ref):
    n_row, n_col, _, tokens, cols = got_ref.shape
    sides = []
    for side in range(2):
        sides.append(
            jnp.concatenate(
                [got_ref[:, x, side].reshape(n_row * tokens, cols) for x in range(n_col)], axis=1
            )
        )
    product = lax.dot_general(sides[0], sides[1], NT, preferred_element_type=f32).astype(bf16)
    for x in range(n_col):
        out_ref[:, x] = product[:, x * cols : (x + 1) * cols].reshape(n_row, tokens, cols)


def triangle(got):
    n_row, n_col, _, tokens, cols = got.shape
    return pl.pallas_call(
        triangle_kernel,
        out_shape=jax.ShapeDtypeStruct((n_row, n_col, tokens, cols), bf16),
        in_specs=[pl.BlockSpec(memory_space=pltpu.VMEM)],
        out_specs=pl.BlockSpec(memory_space=pltpu.VMEM),
        name="triangle",
    )(got)


def doubled(value, axis, bit):
    size = lax.axis_size(axis)
    at = lax.axis_index(axis)
    other = lax.ppermute(value, axis, [(n, n ^ bit) for n in range(size)])
    upper = (at & bit) != 0
    first = jnp.where(upper, other, value)
    second = jnp.where(upper, value, other)
    return jnp.stack([first, second])


def gathered_columns(own):
    n_part = lax.axis_size("part")
    n_col = lax.axis_size("col")
    turned = lax.ppermute(
        own,
        ("part", "col"),
        [(a * n_col + b, b * n_col + a) for a in range(n_part) for b in range(n_col)],
    )
    parts = turned[None]
    bit = lax.axis_size("near") // 2
    order = []
    while bit:
        parts = doubled(parts, "near", bit)
        order.append(bit)
        bit //= 2
    parts = doubled(parts, "core", 1)
    levels = len(order) + 1
    parts = parts.reshape((2,) * levels + own.shape)
    turns = list(range(1, levels)[::-1]) + [0]
    parts = parts.transpose(*turns, levels, levels + 1)
    return parts.reshape(-1, own.shape[1])


def on_device(
    pair_grid,
    alignment_pool,
    sample_index,
    token_mask,
    outer_proj,
    outer_mix,
    pair_logit,
    average_proj,
    average_mix,
    triangle_proj,
    triangle_mix,
    transition_up,
    transition_down,
):
    n_row = lax.axis_size(ROW)
    n_col = lax.axis_size("col")
    tok_row = pair_grid.shape[0]
    tok_col = pair_grid.shape[1]
    pair_width = pair_grid.shape[2]
    samples = sample_index.shape[0]
    align_width = alignment_pool.shape[2]
    outer_width = outer_proj.shape[1] // 2
    head_count = pair_logit.shape[1]
    head_total = average_proj.shape[1] // 2
    head_dim = head_total // head_count
    inner_width = transition_down.shape[0]
    row_start = lax.axis_index(ROW) * tok_row
    column_start = lax.axis_index("col") * tok_col
    quarter = samples // n_col
    sample_start = lax.axis_index("col") * quarter

    alignments = jnp.take(alignment_pool, sample_index, axis=0)
    align_norm = normalize(alignments, 2).astype(bf16)
    norm_t = align_norm.transpose(1, 0, 2)
    norm_rows = gathered_columns(norm_t.reshape(tok_row, samples * align_width))

    group = 16
    mix_d = outer_mix.reshape(outer_width, outer_width, pair_width).transpose(1, 0, 2)
    mixed = mixed_rows(norm_t, outer_proj[:, :outer_width], mix_d, group)
    same = jnp.eye(group, dtype=bf16)
    spread = (
        same[:, None, None, :] * outer_proj[None, :, outer_width:, None]
    ).reshape(group * align_width, outer_width * group)
    row_mask = lax.dynamic_slice_in_dim(token_mask, row_start, tok_row, 0).astype(f32)
    column_mask = lax.dynamic_slice_in_dim(token_mask, column_start, tok_col, 0).astype(f32)
    pair_mask = (row_mask[:, None] * column_mask[None, :])[:, None, :]
    pair_one, pair_norm, weights, factors = pair_part(
        norm_rows, spread, mixed, pair_grid,
        triangle_proj[:, : 4 * pair_width].T, pair_logit.T, pair_mask,
    )

    received = lax.all_to_all(factors, ROW_COL, split_axis=0, concat_axis=0, tiled=True)

    value_weight = average_proj[:, :head_total].reshape(align_width, head_count, head_dim)
    gate_weight = average_proj[:, head_total:]
    partial_total = jnp.sum(weights, axis=2)
    drawn = jnp.dot(
        weights.astype(bf16).reshape(tok_row * head_count, tok_col), norm_rows,
        preferred_element_type=f32,
    ).astype(bf16).reshape(tok_row, head_count, samples, align_width)
    partial_sum = jnp.einsum(
        "ihsm,mhc->sihc", drawn, value_weight, preferred_element_type=f32
    ).astype(bf16).reshape(n_col, quarter, tok_row, head_total)
    high = partial_total.astype(bf16)
    low = (partial_total - high.astype(f32)).astype(bf16)
    total_row = jnp.concatenate([high, low], axis=1)
    total_row = jnp.pad(total_row, ((0, 0), (0, head_total - 2 * head_count)))
    total_row = jnp.broadcast_to(total_row, (n_col, 1, tok_row, head_total))
    sums = jnp.concatenate([partial_sum, total_row], axis=1)
    sums = lax.all_to_all(sums, "col", split_axis=0, concat_axis=0, tiled=True)
    sums = jnp.sum(sums.reshape(n_col, quarter + 1, tok_row, head_total).astype(f32), axis=0)
    totals = sums[quarter, :, :head_count] + sums[quarter, :, head_count : 2 * head_count]
    weighted = sums[:quarter]
    own_norm = lax.dynamic_slice_in_dim(align_norm, sample_start, quarter, 0)
    own_align = lax.dynamic_slice_in_dim(alignments, sample_start, quarter, 0)
    gate_values = jax.nn.sigmoid(
        jnp.einsum("sim,mk->sik", own_norm, gate_weight, preferred_element_type=f32)
    )
    share = jnp.repeat(1.0 / totals, head_dim, axis=1)
    averaged = (gate_values * weighted * share).astype(bf16)
    align_update = jnp.einsum("sik,km->sim", averaged, average_mix, preferred_element_type=f32)
    own_next = (own_align.astype(f32) + align_update).astype(bf16)
    alignment_next = lax.all_gather(own_next, "col", axis=0, tiled=True)

    result = triangle(received.reshape(n_row, n_col, 2, tok_row, tok_col))
    product = lax.all_to_all(
        result.reshape(n_row * n_col, tok_row, tok_col), ROW_COL,
        split_axis=0, concat_axis=0, tiled=True,
    )
    product_norm = normalize(product, 0).astype(bf16).reshape(pair_width, tok_row * tok_col)
    mixed_out = lax.dot_general(product_norm, triangle_mix, TN, preferred_element_type=f32)
    flat_norm = pair_norm.reshape(tok_row * tok_col, pair_width)
    gate_out = jax.nn.sigmoid(
        jnp.dot(flat_norm, triangle_proj[:, 4 * pair_width :], preferred_element_type=f32)
    )
    pair_two = (
        pair_one.reshape(tok_row * tok_col, pair_width).astype(f32) + gate_out * mixed_out
    ).astype(bf16)
    block_rows = 8
    tail_rows = pair_two.reshape(tok_row // block_rows, block_rows * tok_col, pair_width)

    def transition_step(rows_block):
        normed = normalize(rows_block, 1).astype(bf16)
        expanded = jnp.dot(normed, transition_up, preferred_element_type=f32)
        hidden = (jax.nn.silu(expanded[:, :inner_width]) * expanded[:, inner_width:]).astype(bf16)
        return (
            rows_block.astype(f32)
            + jnp.dot(hidden, transition_down, preferred_element_type=f32)
        ).astype(bf16)

    pair_next = lax.map(transition_step, tail_rows).reshape(tok_row, tok_col, pair_width)
    return (pair_next, alignment_next)


def solution(mesh):
    n_groups, n_row, n_col = mesh.shape["groups"], mesh.shape["row"], mesh.shape["col"]
    split = Mesh(
        mesh.devices.reshape(n_groups, n_col, n_row // n_col // 2, 2, n_col),
        ("groups", "part", "near", "core", "col"),
    )
    placed = (
        P(GROUPS_ROW, "col", None),
        P("groups", ROW, None),
        P("groups"),
        P("groups"),
    ) + (P(),) * 9
    return jax.shard_map(
        on_device,
        mesh=split,
        in_specs=placed,
        out_specs=(P(GROUPS_ROW, "col", None), P("groups", ROW, None)),
        check_vma=False,
    )
```

```python
import functools

import jax
import jax.numpy as jnp
from jax import lax
from jax.experimental import pallas as pl
from jax.experimental.pallas import tpu as pltpu
from jax.sharding import Mesh
from jax.sharding import PartitionSpec as P

ROW = ("part", "near", "core")
ROW_COL = ("part", "near", "core", "col")
GROUPS_ROW = ("groups", "part", "near", "core")

epsilon = 1e-05
f32 = jnp.float32
bf16 = jnp.bfloat16
NT = (((1,), (1,)), ((), ()))
TN = (((0,), (0,)), ((), ()))


def normalize(values, channel_dim):
    values = values.astype(f32)
    centred = values - jnp.mean(values, axis=channel_dim, keepdims=True)
    spread = jnp.mean(centred * centred, axis=channel_dim, keepdims=True)
    return centred * lax.rsqrt(spread + epsilon)


def sigmoid(x):
    return 1.0 / (1.0 + jnp.exp(-x))


def whole(shape):
    return pl.BlockSpec(shape, lambda *_: (0,) * len(shape))


def mix_kernel(norm_ref, proj_ref, mix_ref, out_ref, rows_ref, *, scale, group):
    width = mix_ref.shape[2]
    tokens = norm_ref.shape[0]
    samples = norm_ref.shape[1]

    @pl.when(pl.program_id(0) == 0)
    def _():
        flat = norm_ref[...].reshape(tokens * samples, norm_ref.shape[2])
        rows_ref[...] = jnp.dot(flat, proj_ref[...], preferred_element_type=f32).astype(bf16)

    both = jnp.concatenate([mix_ref[0], mix_ref[1]], axis=1)
    part = jnp.dot(rows_ref[...], both, preferred_element_type=f32) * scale
    part = part.astype(bf16)
    for d in range(2):
        for i in range(tokens):
            for g in range(samples // group):
                out_ref[g, d, :, i * width : (i + 1) * width] = part[
                    i * samples + g * group : i * samples + (g + 1) * group,
                    d * width : (d + 1) * width,
                ]


def mixed_rows(norm_t, proj, mix_d, group):
    tokens, samples, _ = norm_t.shape
    depth, inner, width = mix_d.shape
    groups = samples // group
    out = pl.pallas_call(
        functools.partial(mix_kernel, scale=1.0 / samples, group=group),
        grid=(depth // 2,),
        in_specs=[
            whole(norm_t.shape),
            whole(proj.shape),
            pl.BlockSpec((2, inner, width), lambda d: (d, 0, 0)),
        ],
        out_specs=pl.BlockSpec((groups, 2, group, tokens * width), lambda d: (0, d, 0, 0)),
        out_shape=jax.ShapeDtypeStruct((groups, depth, group, tokens * width), bf16),
        scratch_shapes=[pltpu.VMEM((tokens * samples, inner), bf16)],
        cost_estimate=pl.CostEstimate(
            flops=16 * tokens * samples * inner * depth * width,
            bytes_accessed=2 * tokens * samples * depth * width,
            transcendentals=0,
        ),
        name="mixed_rows",
    )(norm_t, proj, mix_d)
    return out.reshape(groups * depth * group, tokens * width)


def pair_kernel(
    order_ref, own_ref, other_ref, spread_ref, mixed_ref, pair_ref, proj_ref, logit_ref, mask_ref,
    one_ref, pnorm_ref, weight_ref, factor_ref, col_ref, left_ref, right_ref,
):
    step = pl.program_id(0)
    rows, cols, width = pair_ref.shape
    tokens = factor_ref.shape[2]
    got, chunk = spread_ref.shape
    held = own_ref.shape[0]

    @pl.when(step == 0)
    def _():
        for half, ref in enumerate((own_ref, other_ref)):
            block = ref[...].reshape(held * tokens, ref.shape[2])
            for g in range(ref.shape[2] // chunk):
                part = lax.dot_general(
                    block[:, g * chunk : (g + 1) * chunk], spread_ref[...], NT,
                    preferred_element_type=f32,
                ).astype(bf16)
                for n in range(held):
                    at = pl.multiple_of(order_ref[half * held + n] * tokens, tokens)
                    col_ref[pl.ds(at, tokens), g * got : (g + 1) * got] = part[
                        n * tokens : (n + 1) * tokens
                    ]

    update = jnp.dot(col_ref[...], mixed_ref[...], preferred_element_type=f32)
    normed = []
    for n in range(rows):
        one = (pair_ref[n].astype(f32) + update[:, n * width : (n + 1) * width]).astype(bf16)
        one_ref[n] = one
        now = normalize(one, 1).astype(bf16)
        pnorm_ref[n] = now
        normed.append(now)
    normed = jnp.concatenate(normed, axis=0)
    projected = lax.dot_general(proj_ref[...], normed, NT, preferred_element_type=f32)
    scores = jnp.exp(lax.dot_general(logit_ref[...], normed, NT, preferred_element_type=f32))
    left = sigmoid(projected[:width]) * projected[width : 2 * width]
    right = sigmoid(projected[2 * width : 3 * width]) * projected[3 * width :]
    for n in range(rows):
        weight_ref[n] = scores[:, n * cols : (n + 1) * cols]
        mask = mask_ref[n]
        lanes = slice(n * cols, (n + 1) * cols)
        at = pl.ds(step * rows + n, width, stride=tokens)
        left_ref[at, :] = left[:, lanes] * mask
        right_ref[at, :] = right[:, lanes] * mask

    @pl.when(step == pl.num_programs(0) - 1)
    def _():
        factor_ref[:, 0] = left_ref[...].reshape(width, tokens, cols).astype(bf16)
        factor_ref[:, 1] = right_ref[...].reshape(width, tokens, cols).astype(bf16)


def pair_part(order, own, other, spread, mixed, pair_grid, proj_t, logit_t, mask):
    tokens, cols, width = pair_grid.shape
    heads = logit_t.shape[0]
    depth = mixed.shape[0]
    rows = 4
    pairs = pl.BlockSpec((rows, cols, width), lambda n, _: (n, 0, 0))
    return pl.pallas_call(
        pair_kernel,
        grid_spec=pltpu.PrefetchScalarGridSpec(
            num_scalar_prefetch=1,
            grid=(tokens // rows,),
            in_specs=[
                whole(own.shape),
                whole(other.shape),
                whole(spread.shape),
                pl.BlockSpec((depth, rows * width), lambda n, _: (0, n)),
                pairs,
                whole(proj_t.shape),
                whole(logit_t.shape),
                pl.BlockSpec((rows, 1, cols), lambda n, _: (n, 0, 0)),
            ],
            out_specs=[
                pairs,
                pairs,
                pl.BlockSpec((rows, heads, cols), lambda n, _: (n, 0, 0)),
                whole((width, 2, tokens, cols)),
            ],
            scratch_shapes=[
                pltpu.VMEM((cols, depth), bf16),
                pltpu.VMEM((width * tokens, cols), f32),
                pltpu.VMEM((width * tokens, cols), f32),
            ],
        ),
        out_shape=[
            jax.ShapeDtypeStruct(pair_grid.shape, bf16),
            jax.ShapeDtypeStruct(pair_grid.shape, bf16),
            jax.ShapeDtypeStruct((tokens, heads, cols), f32),
            jax.ShapeDtypeStruct((width, 2, tokens, cols), bf16),
        ],
        name="pair_part",
    )(order, own, other, spread, mixed, pair_grid, proj_t, logit_t, mask)


def triangle_kernel(got_ref, out_ref):
    n_row, n_col, _, tokens, cols = got_ref.shape
    sides = []
    for side in range(2):
        sides.append(
            jnp.concatenate(
                [got_ref[:, x, side].reshape(n_row * tokens, cols) for x in range(n_col)], axis=1
            )
        )
    product = lax.dot_general(sides[0], sides[1], NT, preferred_element_type=f32).astype(bf16)
    for x in range(n_col):
        out_ref[:, x] = product[:, x * cols : (x + 1) * cols].reshape(n_row, tokens, cols)


def triangle(got):
    n_row, n_col, _, tokens, cols = got.shape
    return pl.pallas_call(
        triangle_kernel,
        out_shape=jax.ShapeDtypeStruct((n_row, n_col, tokens, cols), bf16),
        in_specs=[pl.BlockSpec(memory_space=pltpu.VMEM)],
        out_specs=pl.BlockSpec(memory_space=pltpu.VMEM),
        name="triangle",
    )(got)


def swap(value, axis, bit):
    size = lax.axis_size(axis)
    return lax.ppermute(value, axis, [(n, n ^ bit) for n in range(size)])


def turned_rows(own):
    n_part = lax.axis_size("part")
    n_col = lax.axis_size("col")
    return lax.ppermute(
        own,
        ("part", "col"),
        [(a * n_col + b, b * n_col + a) for a in range(n_part) for b in range(n_col)],
    )


def gathered_pieces(turned):
    near, core = lax.axis_index("near"), lax.axis_index("core")
    parts, codes = turned[None], [0]
    bit = lax.axis_size("near") // 2
    while bit:
        parts = jnp.concatenate([parts, swap(parts, "near", bit)], axis=0)
        codes = codes + [code ^ bit for code in codes]
        bit //= 2
    other = swap(parts, "core", 1)
    order = [(near ^ code) * 2 + core for code in codes]
    order += [(near ^ code) * 2 + 1 - core for code in codes]
    return parts, other, jnp.stack(order).astype(jnp.int32)


def in_order(parts, other):
    near, core = lax.axis_index("near"), lax.axis_index("core")
    count = parts.shape[0]
    levels = count.bit_length() - 1
    both = jnp.stack([parts, other]).reshape((2,) * (levels + 1) + parts.shape[1:])
    both = jnp.where(core == 1, jnp.flip(both, 0), both)
    for level in range(levels):
        bit = (near >> level) & 1
        both = jnp.where(bit == 1, jnp.flip(both, 1 + level), both)
    turns = tuple(range(levels, -1, -1))
    both = both.transpose(*turns, levels + 1, levels + 2)
    return both.reshape(-1, parts.shape[2])


def scattered_sum(value, axis):
    size, at = lax.axis_size(axis), lax.axis_index(axis)
    total = lax.dynamic_index_in_dim(value, at, 0, keepdims=False).astype(f32)
    for k in range(1, size):
        piece = lax.dynamic_index_in_dim(value, (at + k) % size, 0, keepdims=False)
        piece = lax.ppermute(piece, axis, [(n, (n + k) % size) for n in range(size)])
        total = total + piece.astype(f32)
    return total


def on_device(
    pair_grid,
    alignment_pool,
    sample_index,
    token_mask,
    outer_proj,
    outer_mix,
    pair_logit,
    average_proj,
    average_mix,
    triangle_proj,
    triangle_mix,
    transition_up,
    transition_down,
):
    n_row = lax.axis_size(ROW)
    n_col = lax.axis_size("col")
    tok_row = pair_grid.shape[0]
    tok_col = pair_grid.shape[1]
    pair_width = pair_grid.shape[2]
    samples = sample_index.shape[0]
    align_width = alignment_pool.shape[2]
    outer_width = outer_proj.shape[1] // 2
    head_count = pair_logit.shape[1]
    head_total = average_proj.shape[1] // 2
    head_dim = head_total // head_count
    inner_width = transition_down.shape[0]
    row_start = lax.axis_index(ROW) * tok_row
    column_start = lax.axis_index("col") * tok_col
    quarter = samples // n_col
    sample_start = lax.axis_index("col") * quarter

    alignments = jnp.take(alignment_pool, sample_index, axis=0)
    align_norm = normalize(alignments, 2).astype(bf16)
    norm_t = align_norm.transpose(1, 0, 2)
    turned = turned_rows(norm_t.reshape(tok_row, samples * align_width))

    group = 16
    mix_d = outer_mix.reshape(outer_width, outer_width, pair_width).transpose(1, 0, 2)
    mixed = mixed_rows(norm_t, outer_proj[:, :outer_width], mix_d, group)
    same = jnp.eye(group, dtype=bf16)
    spread = (
        same[None, :, :, None] * outer_proj[:, outer_width:].T[:, None, None, :]
    ).reshape(outer_width * group, group * align_width)
    row_mask = lax.dynamic_slice_in_dim(token_mask, row_start, tok_row, 0).astype(f32)
    column_mask = lax.dynamic_slice_in_dim(token_mask, column_start, tok_col, 0).astype(f32)
    pair_mask = (row_mask[:, None] * column_mask[None, :])[:, None, :]
    proj_t, logit_t = triangle_proj[:, : 4 * pair_width].T, pair_logit.T
    turned, mixed, spread, proj_t, logit_t, pair_mask = lax.optimization_barrier(
        (turned, mixed, spread, proj_t, logit_t, pair_mask)
    )
    parts, other, order = gathered_pieces(turned)
    pair_one, pair_norm, weights, factors = pair_part(
        order, parts, other, spread, mixed, pair_grid, proj_t, logit_t, pair_mask
    )

    received = lax.all_to_all(factors, ROW_COL, split_axis=0, concat_axis=0, tiled=True)

    value_weight = average_proj[:, :head_total].reshape(align_width, head_count, head_dim)
    gate_weight = average_proj[:, head_total:]
    partial_total = jnp.sum(weights, axis=2)
    norm_rows = in_order(parts, other)
    drawn = jnp.dot(
        weights.astype(bf16).reshape(tok_row * head_count, tok_col), norm_rows,
        preferred_element_type=f32,
    ).astype(bf16).reshape(tok_row, head_count, samples, align_width)
    partial_sum = jnp.einsum(
        "ihsm,mhc->sihc", drawn, value_weight, preferred_element_type=f32
    ).astype(bf16).reshape(n_col, quarter, tok_row, head_total)
    high = partial_total.astype(bf16)
    low = (partial_total - high.astype(f32)).astype(bf16)
    total_row = jnp.concatenate([high, low], axis=1)
    total_row = jnp.pad(total_row, ((0, 0), (0, head_total - 2 * head_count)))
    total_row = jnp.broadcast_to(total_row, (n_col, 1, tok_row, head_total))
    sums = jnp.concatenate([partial_sum, total_row], axis=1)
    sums = scattered_sum(sums, "col")
    received, sums = lax.optimization_barrier((received, sums))
    totals = sums[quarter, :, :head_count] + sums[quarter, :, head_count : 2 * head_count]
    weighted = sums[:quarter]
    own_norm = lax.dynamic_slice_in_dim(align_norm, sample_start, quarter, 0)
    own_align = lax.dynamic_slice_in_dim(alignments, sample_start, quarter, 0)
    gate_values = jax.nn.sigmoid(
        jnp.einsum("sim,mk->sik", own_norm, gate_weight, preferred_element_type=f32)
    )
    share = jnp.repeat(1.0 / totals, head_dim, axis=1)
    averaged = (gate_values * weighted * share).astype(bf16)
    align_update = jnp.einsum("sik,km->sim", averaged, average_mix, preferred_element_type=f32)
    own_next = (own_align.astype(f32) + align_update).astype(bf16)
    alignment_next = lax.all_gather(own_next, "col", axis=0, tiled=True)

    result = triangle(received.reshape(n_row, n_col, 2, tok_row, tok_col))
    product = lax.all_to_all(
        result.reshape(n_row * n_col, tok_row, tok_col), ROW_COL,
        split_axis=0, concat_axis=0, tiled=True,
    )
    product_norm = normalize(product, 0).astype(bf16).reshape(pair_width, tok_row * tok_col)
    mixed_out = lax.dot_general(product_norm, triangle_mix, TN, preferred_element_type=f32)
    flat_norm = pair_norm.reshape(tok_row * tok_col, pair_width)
    gate_out = jax.nn.sigmoid(
        jnp.dot(flat_norm, triangle_proj[:, 4 * pair_width :], preferred_element_type=f32)
    )
    pair_two = (
        pair_one.reshape(tok_row * tok_col, pair_width).astype(f32) + gate_out * mixed_out
    ).astype(bf16)
    block_rows = 8
    tail_rows = pair_two.reshape(tok_row // block_rows, block_rows * tok_col, pair_width)

    def transition_step(rows_block):
        normed = normalize(rows_block, 1).astype(bf16)
        expanded = jnp.dot(normed, transition_up, preferred_element_type=f32)
        hidden = (jax.nn.silu(expanded[:, :inner_width]) * expanded[:, inner_width:]).astype(bf16)
        return (
            rows_block.astype(f32)
            + jnp.dot(hidden, transition_down, preferred_element_type=f32)
        ).astype(bf16)

    pair_next = lax.map(transition_step, tail_rows).reshape(tok_row, tok_col, pair_width)
    return (pair_next, alignment_next)


def solution(mesh):
    n_groups, n_row, n_col = mesh.shape["groups"], mesh.shape["row"], mesh.shape["col"]
    split = Mesh(
        mesh.devices.reshape(n_groups, n_col, n_row // n_col // 2, 2, n_col),
        ("groups", "part", "near", "core", "col"),
    )
    placed = (
        P(GROUPS_ROW, "col", None),
        P("groups", ROW, None),
        P("groups"),
        P("groups"),
    ) + (P(),) * 9
    return jax.shard_map(
        on_device,
        mesh=split,
        in_specs=placed,
        out_specs=(P(GROUPS_ROW, "col", None), P("groups", ROW, None)),
        check_vma=False,
    )
```

```python
import functools

import jax
import jax.numpy as jnp
from jax import lax
from jax.experimental import pallas as pl
from jax.experimental.pallas import tpu as pltpu
from jax.sharding import Mesh
from jax.sharding import PartitionSpec as P

ROW = ("part", "near", "core")
ROW_COL = ("part", "near", "core", "col")
GROUPS_ROW = ("groups", "part", "near", "core")

epsilon = 1e-05
f32 = jnp.float32
bf16 = jnp.bfloat16
NT = (((1,), (1,)), ((), ()))
TN = (((0,), (0,)), ((), ()))


def normalize(values, channel_dim):
    values = values.astype(f32)
    centred = values - jnp.mean(values, axis=channel_dim, keepdims=True)
    spread = jnp.mean(centred * centred, axis=channel_dim, keepdims=True)
    return centred * lax.rsqrt(spread + epsilon)


def sigmoid(x):
    return 1.0 / (1.0 + jnp.exp(-x))


def limit(mebibytes):
    return pltpu.CompilerParams(vmem_limit_bytes=mebibytes * 1024 * 1024)


def whole(shape):
    return pl.BlockSpec(shape, lambda *_: (0,) * len(shape))


def draw_kernel(index_ref, pool_ref, drawn_ref, norm_ref, flat_ref, turn_ref, turned_ref, sem):
    samples, tokens, width = drawn_ref.shape

    def start(s, carry):
        pltpu.make_async_copy(pool_ref.at[index_ref[s]], drawn_ref.at[s], sem.at[s]).start()
        return carry

    def finish(s, carry):
        pltpu.make_async_copy(pool_ref.at[index_ref[s]], drawn_ref.at[s], sem.at[s]).wait()
        return carry

    lax.fori_loop(0, samples, start, 0)
    lax.fori_loop(0, samples, finish, 0)
    normed = normalize(drawn_ref[...], 2)
    norm_ref[...] = normed.astype(bf16)
    for s in range(0, samples, 2):
        both = jnp.concatenate([normed[s], normed[s + 1]], axis=1)
        flat_ref[:, s * width : (s + 2) * width] = both.astype(bf16)
        turned_ref[pl.ds(s, tokens, stride=samples), :] = normed[s]
        turned_ref[pl.ds(s + 1, tokens, stride=samples), :] = normed[s + 1]
    turn_ref[...] = turned_ref[...].reshape(tokens, samples, width).astype(bf16)


def drawn_alignments(pool, index):
    _, tokens, width = pool.shape
    samples = index.shape[0]
    vmem = pl.BlockSpec(memory_space=pltpu.VMEM)
    return pl.pallas_call(
        draw_kernel,
        in_specs=[pl.BlockSpec(memory_space=pltpu.SMEM), pl.BlockSpec(memory_space=pl.ANY)],
        out_specs=[vmem] * 4,
        out_shape=[
            jax.ShapeDtypeStruct((samples, tokens, width), bf16),
            jax.ShapeDtypeStruct((samples, tokens, width), bf16),
            jax.ShapeDtypeStruct((tokens, samples * width), bf16),
            jax.ShapeDtypeStruct((tokens, samples, width), bf16),
        ],
        scratch_shapes=[
            pltpu.VMEM((tokens * samples, width), f32),
            pltpu.SemaphoreType.DMA((samples,)),
        ],
        compiler_params=limit(8),
        name="draw",
    )(index, pool)


def mix_kernel(norm_ref, proj_ref, mix_ref, out_ref, rows_ref, *, scale, group):
    width = mix_ref.shape[2]
    tokens = norm_ref.shape[0]
    samples = norm_ref.shape[1]

    @pl.when(pl.program_id(0) == 0)
    def _():
        flat = norm_ref[...].reshape(tokens * samples, norm_ref.shape[2])
        rows_ref[...] = jnp.dot(flat, proj_ref[...], preferred_element_type=f32).astype(bf16)

    both = jnp.concatenate([mix_ref[0], mix_ref[1]], axis=1)
    half = tokens * samples // 2
    step = pl.program_id(0) * 2
    for top in range(2):
        part = jnp.dot(
            rows_ref[top * half : (top + 1) * half], both, preferred_element_type=f32
        ) * scale
        part = part.astype(bf16)
        for d in range(2):
            for i in range(tokens // 2):
                at = (top * (tokens // 2) + i) * width
                for g in range(samples // group):
                    out_ref[g, step + d, :, at : at + width] = part[
                        i * samples + g * group : i * samples + (g + 1) * group,
                        d * width : (d + 1) * width,
                    ]


def mixed_rows(norm_t, proj, mix_d, group):
    tokens, samples, _ = norm_t.shape
    depth, inner, width = mix_d.shape
    groups = samples // group
    out = pl.pallas_call(
        functools.partial(mix_kernel, scale=1.0 / samples, group=group),
        grid=(depth // 2,),
        in_specs=[
            whole(norm_t.shape),
            whole(proj.shape),
            pl.BlockSpec((2, inner, width), lambda d: (d, 0, 0)),
        ],
        out_specs=pl.BlockSpec(memory_space=pltpu.VMEM),
        out_shape=jax.ShapeDtypeStruct((groups, depth, group, tokens * width), bf16),
        scratch_shapes=[pltpu.VMEM((tokens * samples, inner), bf16)],
        cost_estimate=pl.CostEstimate(
            flops=16 * tokens * samples * inner * depth * width,
            bytes_accessed=2 * tokens * samples * depth * width,
            transcendentals=0,
        ),
        compiler_params=limit(16),
        name="mixed_rows",
    )(norm_t, proj, mix_d)
    return out.reshape(groups * depth * group, tokens * width)


def pair_kernel(
    place_ref, own_ref, other_ref, spread_ref, mixed_ref, pair_ref, proj_ref, logit_ref, mask_ref,
    one_ref, pnorm_ref, weight_ref, factor_ref, col_ref, left_ref, right_ref, *, codes,
):
    step = pl.program_id(0)
    rows, cols, width = pair_ref.shape
    tokens = factor_ref.shape[2]
    got, chunk = spread_ref.shape
    held = own_ref.shape[0]

    @pl.when(step == 0)
    def _():
        block = jnp.concatenate(
            [ref[...].reshape(held * tokens, ref.shape[2]) for ref in (own_ref, other_ref)], axis=0
        )
        for g in range(block.shape[1] // chunk):
            part = lax.dot_general(
                block[:, g * chunk : (g + 1) * chunk], spread_ref[...], NT,
                preferred_element_type=f32,
            ).astype(bf16)
            for n, code in enumerate(codes):
                at = pl.multiple_of((place_ref[0] ^ code) * tokens, tokens)
                col_ref[pl.ds(at, tokens), g * got : (g + 1) * got] = part[
                    n * tokens : (n + 1) * tokens
                ]

    lanes = pl.ds(pl.multiple_of(step * rows * width, rows * width), rows * width)
    update = jnp.dot(col_ref[...], mixed_ref[:, lanes], preferred_element_type=f32)
    normed = []
    for n in range(rows):
        one = (pair_ref[n].astype(f32) + update[:, n * width : (n + 1) * width]).astype(bf16)
        one_ref[n] = one
        now = normalize(one, 1).astype(bf16)
        pnorm_ref[n] = now
        normed.append(now)
    normed = jnp.concatenate(normed, axis=0)
    projected = lax.dot_general(proj_ref[...], normed, NT, preferred_element_type=f32)
    scores = jnp.exp(lax.dot_general(logit_ref[...], normed, NT, preferred_element_type=f32))
    left = sigmoid(projected[:width]) * projected[width : 2 * width]
    right = sigmoid(projected[2 * width : 3 * width]) * projected[3 * width :]
    for n in range(rows):
        weight_ref[n] = scores[:, n * cols : (n + 1) * cols]
        mask = mask_ref[n]
        lanes = slice(n * cols, (n + 1) * cols)
        at = pl.ds(step * rows + n, width, stride=tokens)
        left_ref[at, :] = left[:, lanes] * mask
        right_ref[at, :] = right[:, lanes] * mask

    @pl.when(step == pl.num_programs(0) - 1)
    def _():
        factor_ref[:, 0] = left_ref[...].reshape(width, tokens, cols).astype(bf16)
        factor_ref[:, 1] = right_ref[...].reshape(width, tokens, cols).astype(bf16)


def pair_part(place, codes, own, other, spread, mixed, pair_grid, proj_t, logit_t, mask):
    tokens, cols, width = pair_grid.shape
    heads = logit_t.shape[0]
    depth = mixed.shape[0]
    rows = 4
    pairs = pl.BlockSpec((rows, cols, width), lambda n, _: (n, 0, 0))
    return pl.pallas_call(
        functools.partial(pair_kernel, codes=codes),
        grid_spec=pltpu.PrefetchScalarGridSpec(
            num_scalar_prefetch=1,
            grid=(tokens // rows,),
            in_specs=[
                whole(own.shape),
                whole(other.shape),
                whole(spread.shape),
                pl.BlockSpec(memory_space=pltpu.VMEM),
                pairs,
                whole(proj_t.shape),
                whole(logit_t.shape),
                pl.BlockSpec((rows, 1, cols), lambda n, _: (n, 0, 0)),
            ],
            out_specs=[
                pairs,
                pairs,
                pl.BlockSpec((rows, heads, cols), lambda n, _: (n, 0, 0)),
                whole((width, 2, tokens, cols)),
            ],
            scratch_shapes=[
                pltpu.VMEM((cols, depth), bf16),
                pltpu.VMEM((width * tokens, cols), f32),
                pltpu.VMEM((width * tokens, cols), f32),
            ],
        ),
        out_shape=[
            jax.ShapeDtypeStruct(pair_grid.shape, bf16),
            jax.ShapeDtypeStruct(pair_grid.shape, bf16),
            jax.ShapeDtypeStruct((tokens, heads, cols), f32),
            jax.ShapeDtypeStruct((width, 2, tokens, cols), bf16),
        ],
        compiler_params=limit(32),
        name="pair_part",
    )(place, own, other, spread, mixed, pair_grid, proj_t, logit_t, mask)


def triangle_kernel(got_ref, out_ref):
    n_row, n_col, _, tokens, cols = got_ref.shape
    sides = []
    for side in range(2):
        sides.append(
            jnp.concatenate(
                [got_ref[:, x, side].reshape(n_row * tokens, cols) for x in range(n_col)], axis=1
            )
        )
    product = lax.dot_general(sides[0], sides[1], NT, preferred_element_type=f32).astype(bf16)
    for x in range(n_col):
        out_ref[:, x] = product[:, x * cols : (x + 1) * cols].reshape(n_row, tokens, cols)


def triangle(got):
    n_row, n_col, _, tokens, cols = got.shape
    return pl.pallas_call(
        triangle_kernel,
        out_shape=jax.ShapeDtypeStruct((n_row, n_col, tokens, cols), bf16),
        in_specs=[pl.BlockSpec(memory_space=pltpu.VMEM)],
        out_specs=pl.BlockSpec(memory_space=pltpu.VMEM),
        compiler_params=limit(16),
        name="triangle",
    )(got)


def tail_kernel(product_ref, one_ref, gate_ref, mix_ref, up_ref, down_ref, out_ref, turned_ref):
    step = pl.program_id(0)
    rows, cols, width = one_ref.shape
    _, tokens, _ = product_ref.shape
    inner = down_ref.shape[0]

    @pl.when(step == 0)
    def _():
        turned_ref[...] = normalize(product_ref[...], 0).reshape(width * tokens, cols)

    pair_two = []
    for n in range(rows):
        block = turned_ref[pl.ds(step * rows + n, width, stride=tokens), :].astype(bf16)
        mixed = lax.dot_general(block, mix_ref[...], TN, preferred_element_type=f32)
        pair_two.append((one_ref[n].astype(f32) + gate_ref[n] * mixed).astype(bf16))
    pair_two = jnp.concatenate(pair_two, axis=0)
    normed = normalize(pair_two, 1).astype(bf16)
    first = jnp.dot(normed, up_ref[:, :inner], preferred_element_type=f32)
    second = jnp.dot(normed, up_ref[:, inner:], preferred_element_type=f32)
    hidden = (first * sigmoid(first) * second).astype(bf16)
    update = jnp.dot(hidden, down_ref[...], preferred_element_type=f32)
    out_ref[...] = (pair_two.astype(f32) + update).astype(bf16).reshape(rows, cols, width)


def tail(product, one, gate, mix, up, down):
    tokens, cols, width = one.shape
    rows = 4
    pairs = pl.BlockSpec((rows, cols, width), lambda n: (n, 0, 0))
    return pl.pallas_call(
        tail_kernel,
        grid=(tokens // rows,),
        in_specs=[whole(product.shape), pairs, pairs, whole(mix.shape), whole(up.shape), whole(down.shape)],
        out_specs=pairs,
        out_shape=jax.ShapeDtypeStruct(one.shape, bf16),
        scratch_shapes=[pltpu.VMEM((width * tokens, cols), f32)],
        compiler_params=limit(24),
        name="tail",
    )(product, one, gate, mix, up, down)


def swap(value, axis, bit):
    size = lax.axis_size(axis)
    return lax.ppermute(value, axis, [(n, n ^ bit) for n in range(size)])


def turned_rows(own):
    n_part = lax.axis_size("part")
    n_col = lax.axis_size("col")
    return lax.ppermute(
        own,
        ("part", "col"),
        [(a * n_col + b, b * n_col + a) for a in range(n_part) for b in range(n_col)],
    )


def gathered_pieces(turned):
    near, core = lax.axis_index("near"), lax.axis_index("core")
    parts, codes = turned[None], [0]
    bit = lax.axis_size("near") // 2
    while bit:
        parts = jnp.concatenate([parts, swap(parts, "near", bit)], axis=0)
        codes = codes + [code ^ bit for code in codes]
        bit //= 2
    other = swap(parts, "core", 1)
    place = (near * 2 + core).astype(jnp.int32).reshape(1)
    codes = [code * 2 for code in codes] + [code * 2 + 1 for code in codes]
    return parts, other, place, codes


def in_order(parts, other):
    near, core = lax.axis_index("near"), lax.axis_index("core")
    count = parts.shape[0]
    levels = count.bit_length() - 1
    both = jnp.stack([parts, other]).reshape((2,) * (levels + 1) + parts.shape[1:])
    both = jnp.where(core == 1, jnp.flip(both, 0), both)
    for level in range(levels):
        bit = (near >> level) & 1
        both = jnp.where(bit == 1, jnp.flip(both, 1 + level), both)
    turns = tuple(range(levels, -1, -1))
    both = both.transpose(*turns, levels + 1, levels + 2)
    return both.reshape(-1, parts.shape[2])


def scattered_sum(value, axis):
    size, at = lax.axis_size(axis), lax.axis_index(axis)
    total = lax.dynamic_index_in_dim(value, at, 0, keepdims=False).astype(f32)
    for k in range(1, size):
        piece = lax.dynamic_index_in_dim(value, (at + k) % size, 0, keepdims=False)
        piece = lax.ppermute(piece, axis, [(n, (n + k) % size) for n in range(size)])
        total = total + piece.astype(f32)
    return total


def on_device(
    pair_grid,
    alignment_pool,
    sample_index,
    token_mask,
    outer_proj,
    outer_mix,
    pair_logit,
    average_proj,
    average_mix,
    triangle_proj,
    triangle_mix,
    transition_up,
    transition_down,
):
    n_row = lax.axis_size(ROW)
    n_col = lax.axis_size("col")
    tok_row = pair_grid.shape[0]
    tok_col = pair_grid.shape[1]
    pair_width = pair_grid.shape[2]
    samples = sample_index.shape[0]
    align_width = alignment_pool.shape[2]
    outer_width = outer_proj.shape[1] // 2
    head_count = pair_logit.shape[1]
    head_total = average_proj.shape[1] // 2
    head_dim = head_total // head_count
    row_start = lax.axis_index(ROW) * tok_row
    column_start = lax.axis_index("col") * tok_col
    quarter = samples // n_col
    sample_start = lax.axis_index("col") * quarter

    alignments, align_norm, norm_flat, norm_t = drawn_alignments(alignment_pool, sample_index)
    turned = turned_rows(norm_flat)

    group = 16
    mix_d = outer_mix.reshape(outer_width, outer_width, pair_width).transpose(1, 0, 2)
    mixed = mixed_rows(norm_t, outer_proj[:, :outer_width], mix_d, group)
    same = jnp.eye(group, dtype=bf16)
    spread = (
        same[None, :, :, None] * outer_proj[:, outer_width:].T[:, None, None, :]
    ).reshape(outer_width * group, group * align_width)
    row_mask = lax.dynamic_slice_in_dim(token_mask, row_start, tok_row, 0).astype(f32)
    column_mask = lax.dynamic_slice_in_dim(token_mask, column_start, tok_col, 0).astype(f32)
    pair_mask = (row_mask[:, None] * column_mask[None, :])[:, None, :]
    proj_t, logit_t = triangle_proj[:, : 4 * pair_width].T, pair_logit.T
    turned, mixed, spread, proj_t, logit_t, pair_mask = lax.optimization_barrier(
        (turned, mixed, spread, proj_t, logit_t, pair_mask)
    )
    parts, other, place, codes = gathered_pieces(turned)
    pair_one, pair_norm, weights, factors = pair_part(
        place, codes, parts, other, spread, mixed, pair_grid, proj_t, logit_t, pair_mask
    )

    factors, parts, other = lax.optimization_barrier((factors, parts, other))
    received = lax.all_to_all(factors, ROW_COL, split_axis=0, concat_axis=0, tiled=True)

    value_weight = average_proj[:, :head_total].reshape(align_width, head_count, head_dim)
    gate_weight = average_proj[:, head_total:]
    partial_total = jnp.sum(weights, axis=2)
    norm_rows = in_order(parts, other)
    drawn = jnp.dot(
        weights.astype(bf16).reshape(tok_row * head_count, tok_col), norm_rows,
        preferred_element_type=f32,
    ).astype(bf16).reshape(tok_row, head_count, samples, align_width)
    partial_sum = jnp.einsum(
        "ihsm,mhc->sihc", drawn, value_weight, preferred_element_type=f32
    ).astype(bf16).reshape(n_col, quarter, tok_row, head_total)
    high = partial_total.astype(bf16)
    low = (partial_total - high.astype(f32)).astype(bf16)
    total_row = jnp.concatenate([high, low], axis=1)
    total_row = jnp.pad(total_row, ((0, 0), (0, head_total - 2 * head_count)))
    total_row = jnp.broadcast_to(total_row, (n_col, 1, tok_row, head_total))
    sums = jnp.concatenate([partial_sum, total_row], axis=1)
    sums = scattered_sum(sums, "col")
    received, sums = lax.optimization_barrier((received, sums))
    totals = sums[quarter, :, :head_count] + sums[quarter, :, head_count : 2 * head_count]
    weighted = sums[:quarter]
    own_norm = lax.dynamic_slice_in_dim(align_norm, sample_start, quarter, 0)
    own_align = lax.dynamic_slice_in_dim(alignments, sample_start, quarter, 0)
    gate_values = jax.nn.sigmoid(
        jnp.einsum("sim,mk->sik", own_norm, gate_weight, preferred_element_type=f32)
    )
    share = jnp.repeat(1.0 / totals, head_dim, axis=1)
    averaged = (gate_values * weighted * share).astype(bf16)
    align_update = jnp.einsum("sik,km->sim", averaged, average_mix, preferred_element_type=f32)
    own_next = (own_align.astype(f32) + align_update).astype(bf16)
    alignment_next = lax.all_gather(own_next, "col", axis=0, tiled=True)

    result = triangle(received.reshape(n_row, n_col, 2, tok_row, tok_col))
    product = lax.all_to_all(
        result.reshape(n_row * n_col, tok_row, tok_col), ROW_COL,
        split_axis=0, concat_axis=0, tiled=True,
    )
    flat_norm = pair_norm.reshape(tok_row * tok_col, pair_width)
    gate_out = jax.nn.sigmoid(
        jnp.dot(flat_norm, triangle_proj[:, 4 * pair_width :], preferred_element_type=f32)
    ).reshape(pair_grid.shape)
    pair_next = tail(product, pair_one, gate_out, triangle_mix, transition_up, transition_down)
    return (pair_next, alignment_next)


def solution(mesh):
    n_groups, n_row, n_col = mesh.shape["groups"], mesh.shape["row"], mesh.shape["col"]
    split = Mesh(
        mesh.devices.reshape(n_groups, n_col, n_row // n_col // 2, 2, n_col),
        ("groups", "part", "near", "core", "col"),
    )
    placed = (
        P(GROUPS_ROW, "col", None),
        P("groups", ROW, None),
        P("groups"),
        P("groups"),
    ) + (P(),) * 9
    return jax.shard_map(
        on_device,
        mesh=split,
        in_specs=placed,
        out_specs=(P(GROUPS_ROW, "col", None), P("groups", ROW, None)),
        check_vma=False,
    )
```

```python
import functools

import jax
import jax.numpy as jnp
from jax import lax
from jax.experimental import pallas as pl
from jax.experimental.pallas import tpu as pltpu
from jax.sharding import Mesh
from jax.sharding import PartitionSpec as P

ROW = ("part", "near", "core")
ROW_COL = ("part", "near", "core", "col")
GROUPS_ROW = ("groups", "part", "near", "core")

epsilon = 1e-05
f32 = jnp.float32
bf16 = jnp.bfloat16
NT = (((1,), (1,)), ((), ()))
TN = (((0,), (0,)), ((), ()))


def normalize(values, channel_dim):
    values = values.astype(f32)
    centred = values - jnp.mean(values, axis=channel_dim, keepdims=True)
    spread = jnp.mean(centred * centred, axis=channel_dim, keepdims=True)
    return centred * lax.rsqrt(spread + epsilon)


def sigmoid(x):
    return 1.0 / (1.0 + jnp.exp(-x))


def whole(shape):
    return pl.BlockSpec(shape, lambda *_: (0,) * len(shape))


def draw_kernel(index_ref, pool_ref, turn_ref, flat_ref, normed_ref):
    tokens, samples, width = turn_ref.shape
    stored = pool_ref.shape[2]
    at = lax.broadcasted_iota(jnp.int32, (stored, samples), 0)
    pick = jnp.where(at == index_ref[...], 1.0, 0.0).astype(f32).T.astype(bf16)
    for t in range(tokens):
        drawn = lax.dot_general(pick, pool_ref[t], NT, preferred_element_type=f32)
        normed = normalize(drawn, 1)
        turn_ref[t] = normed.astype(bf16)
        normed_ref[t * samples : (t + 1) * samples, :] = normed
    for s in range(0, samples, 2):
        both = jnp.concatenate(
            [normed_ref[pl.ds(s + n, tokens, stride=samples), :] for n in range(2)], axis=1
        )
        flat_ref[:, s * width : (s + 2) * width] = both.astype(bf16)


def drawn_alignments(pool, index):
    _, tokens, width = pool.shape
    samples = index.shape[0]
    vmem = pl.BlockSpec(memory_space=pltpu.VMEM)
    return pl.pallas_call(
        draw_kernel,
        in_specs=[vmem] * 2,
        out_specs=[vmem] * 2,
        out_shape=[
            jax.ShapeDtypeStruct((tokens, samples, width), bf16),
            jax.ShapeDtypeStruct((tokens, samples * width), bf16),
        ],
        scratch_shapes=[pltpu.VMEM((tokens * samples, width), f32)],
        name="draw",
    )(index.reshape(1, samples), pool.transpose(1, 2, 0))


def mix_kernel(norm_ref, proj_ref, mix_ref, out_ref, rows_ref, *, scale, group):
    width = mix_ref.shape[2]
    tokens = norm_ref.shape[0]
    samples = norm_ref.shape[1]

    @pl.when(pl.program_id(0) == 0)
    def _():
        flat = norm_ref[...].reshape(tokens * samples, norm_ref.shape[2])
        rows_ref[...] = jnp.dot(flat, proj_ref[...], preferred_element_type=f32).astype(bf16)

    both = jnp.concatenate([mix_ref[0], mix_ref[1]], axis=1)
    half = tokens * samples // 2
    rows = out_ref.shape[4] // width
    for top in range(2):
        part = jnp.dot(
            rows_ref[top * half : (top + 1) * half], both, preferred_element_type=f32
        ) * scale
        part = part.astype(bf16)
        for d in range(2):
            for n in range(tokens // 2):
                i = top * (tokens // 2) + n
                at = (i % rows) * width
                for g in range(samples // group):
                    out_ref[i // rows, g, d, :, at : at + width] = part[
                        n * samples + g * group : n * samples + (g + 1) * group,
                        d * width : (d + 1) * width,
                    ]


def mixed_rows(norm_t, proj, mix_d, group, rows):
    tokens, samples, _ = norm_t.shape
    depth, inner, width = mix_d.shape
    outer = (tokens // rows, samples // group)
    inside = (group, rows * width)
    out = pl.pallas_call(
        functools.partial(mix_kernel, scale=1.0 / samples, group=group),
        grid=(depth // 2,),
        in_specs=[
            whole(norm_t.shape),
            whole(proj.shape),
            pl.BlockSpec((2, inner, width), lambda d: (d, 0, 0)),
        ],
        out_specs=pl.BlockSpec(outer + (2,) + inside, lambda d: (0, 0, d, 0, 0)),
        out_shape=jax.ShapeDtypeStruct(outer + (depth,) + inside, bf16),
        scratch_shapes=[pltpu.VMEM((tokens * samples, inner), bf16)],
        cost_estimate=pl.CostEstimate(
            flops=16 * tokens * samples * inner * depth * width,
            bytes_accessed=2 * tokens * samples * depth * width,
            transcendentals=0,
        ),
        name="mixed_rows",
    )(norm_t, proj, mix_d)
    return out.reshape(tokens // rows, samples * depth, rows * width)


def pair_kernel(
    place_ref, own_ref, other_ref, spread_ref, mixed_ref, pair_ref, proj_ref, logit_ref, mask_ref,
    one_ref, pnorm_ref, weight_ref, factor_ref, col_ref, left_ref, right_ref, *, codes,
):
    step = pl.program_id(0)
    rows, cols, width = pair_ref.shape
    tokens = factor_ref.shape[2]
    got, chunk = spread_ref.shape
    held = own_ref.shape[0]

    @pl.when(step == 0)
    def _():
        block = jnp.concatenate(
            [ref[...].reshape(held * tokens, ref.shape[2]) for ref in (own_ref, other_ref)], axis=0
        )
        for g in range(block.shape[1] // chunk):
            part = lax.dot_general(
                block[:, g * chunk : (g + 1) * chunk], spread_ref[...], NT,
                preferred_element_type=f32,
            ).astype(bf16)
            for n, code in enumerate(codes):
                at = pl.multiple_of((place_ref[0] ^ code) * tokens, tokens)
                col_ref[pl.ds(at, tokens), g * got : (g + 1) * got] = part[
                    n * tokens : (n + 1) * tokens
                ]

    update = jnp.dot(col_ref[...], mixed_ref[0], preferred_element_type=f32)
    normed = []
    for n in range(rows):
        one = (pair_ref[n].astype(f32) + update[:, n * width : (n + 1) * width]).astype(bf16)
        one_ref[n] = one
        now = normalize(one, 1).astype(bf16)
        pnorm_ref[n] = now
        normed.append(now)
    normed = jnp.concatenate(normed, axis=0)
    projected = lax.dot_general(proj_ref[...], normed, NT, preferred_element_type=f32)
    scores = jnp.exp(lax.dot_general(logit_ref[...], normed, NT, preferred_element_type=f32))
    left = sigmoid(projected[:width]) * projected[width : 2 * width]
    right = sigmoid(projected[2 * width : 3 * width]) * projected[3 * width :]
    for n in range(rows):
        weight_ref[n] = scores[:, n * cols : (n + 1) * cols]
        mask = mask_ref[n]
        lanes = slice(n * cols, (n + 1) * cols)
        at = pl.ds(step * rows + n, width, stride=tokens)
        left_ref[at, :] = left[:, lanes] * mask
        right_ref[at, :] = right[:, lanes] * mask

    @pl.when(step == pl.num_programs(0) - 1)
    def _():
        factor_ref[:, 0] = left_ref[...].reshape(width, tokens, cols).astype(bf16)
        factor_ref[:, 1] = right_ref[...].reshape(width, tokens, cols).astype(bf16)


def pair_part(place, codes, own, other, spread, mixed, pair_grid, proj_t, logit_t, mask):
    tokens, cols, width = pair_grid.shape
    heads = logit_t.shape[0]
    depth = mixed.shape[1]
    rows = mixed.shape[2] // width
    pairs = pl.BlockSpec((rows, cols, width), lambda n, _: (n, 0, 0))
    return pl.pallas_call(
        functools.partial(pair_kernel, codes=codes),
        grid_spec=pltpu.PrefetchScalarGridSpec(
            num_scalar_prefetch=1,
            grid=(tokens // rows,),
            in_specs=[
                whole(own.shape),
                whole(other.shape),
                whole(spread.shape),
                pl.BlockSpec((1, depth, rows * width), lambda n, _: (n, 0, 0)),
                pairs,
                whole(proj_t.shape),
                whole(logit_t.shape),
                pl.BlockSpec((rows, 1, cols), lambda n, _: (n, 0, 0)),
            ],
            out_specs=[
                pairs,
                pairs,
                pl.BlockSpec((rows, heads, cols), lambda n, _: (n, 0, 0)),
                whole((width, 2, tokens, cols)),
            ],
            scratch_shapes=[
                pltpu.VMEM((cols, depth), bf16),
                pltpu.VMEM((width * tokens, cols), f32),
                pltpu.VMEM((width * tokens, cols), f32),
            ],
        ),
        out_shape=[
            jax.ShapeDtypeStruct(pair_grid.shape, bf16),
            jax.ShapeDtypeStruct(pair_grid.shape, bf16),
            jax.ShapeDtypeStruct((tokens, heads, cols), f32),
            jax.ShapeDtypeStruct((width, 2, tokens, cols), bf16),
        ],
        name="pair_part",
    )(place, own, other, spread, mixed, pair_grid, proj_t, logit_t, mask)


def triangle_kernel(got_ref, out_ref):
    n_row, n_col, _, tokens, cols = got_ref.shape
    sides = []
    for side in range(2):
        sides.append(
            jnp.concatenate(
                [got_ref[:, x, side].reshape(n_row * tokens, cols) for x in range(n_col)], axis=1
            )
        )
    product = lax.dot_general(sides[0], sides[1], NT, preferred_element_type=f32).astype(bf16)
    for x in range(n_col):
        out_ref[:, x] = product[:, x * cols : (x + 1) * cols].reshape(n_row, tokens, cols)


def triangle(got):
    n_row, n_col, _, tokens, cols = got.shape
    return pl.pallas_call(
        triangle_kernel,
        out_shape=jax.ShapeDtypeStruct((n_row, n_col, tokens, cols), bf16),
        in_specs=[pl.BlockSpec(memory_space=pltpu.VMEM)],
        out_specs=pl.BlockSpec(memory_space=pltpu.VMEM),
        name="triangle",
    )(got)


def tail_kernel(
    product_ref, one_ref, gate_ref, mix_ref, up_ref, down_ref, next_ref,
    out_ref, copied_ref, turned_ref,
):
    step = pl.program_id(0)
    rows, cols, width = one_ref.shape
    _, tokens, _ = product_ref.shape
    inner = down_ref.shape[0]

    @pl.when(step == 0)
    def _():
        turned_ref[...] = normalize(product_ref[...], 0).reshape(width * tokens, cols)
        copied_ref[...] = next_ref[...]

    pair_two = []
    for n in range(rows):
        block = turned_ref[pl.ds(step * rows + n, width, stride=tokens), :].astype(bf16)
        mixed = lax.dot_general(block, mix_ref[...], TN, preferred_element_type=f32)
        pair_two.append((one_ref[n].astype(f32) + gate_ref[n] * mixed).astype(bf16))
    pair_two = jnp.concatenate(pair_two, axis=0)
    normed = normalize(pair_two, 1).astype(bf16)
    first = jnp.dot(normed, up_ref[:, :inner], preferred_element_type=f32)
    second = jnp.dot(normed, up_ref[:, inner:], preferred_element_type=f32)
    hidden = (first * sigmoid(first) * second).astype(bf16)
    update = jnp.dot(hidden, down_ref[...], preferred_element_type=f32)
    out_ref[...] = (pair_two.astype(f32) + update).astype(bf16).reshape(rows, cols, width)


def tail(product, one, gate, mix, up, down, following):
    tokens, cols, width = one.shape
    rows = 4
    pairs = pl.BlockSpec((rows, cols, width), lambda n: (n, 0, 0))
    return pl.pallas_call(
        tail_kernel,
        grid=(tokens // rows,),
        in_specs=[
            whole(product.shape), pairs, pairs, whole(mix.shape), whole(up.shape),
            whole(down.shape), whole(following.shape),
        ],
        out_specs=[pairs, whole(following.shape)],
        out_shape=[
            jax.ShapeDtypeStruct(one.shape, bf16),
            jax.ShapeDtypeStruct(following.shape, bf16),
        ],
        scratch_shapes=[pltpu.VMEM((width * tokens, cols), f32)],
        compiler_params=pltpu.CompilerParams(vmem_limit_bytes=24 * 1024 * 1024),
        name="tail",
    )(product, one, gate, mix, up, down, following)


def swap(value, axis, bit):
    size = lax.axis_size(axis)
    return lax.ppermute(value, axis, [(n, n ^ bit) for n in range(size)])


def flipped(part, col, n_part, n_near):
    return jnp.where((part - col) % n_part * 2 == n_part, n_near - 1, 0)


def turned_rows(own):
    n_part, n_near = lax.axis_size("part"), lax.axis_size("near")
    pairs = []
    for a in range(n_part):
        for n in range(n_near):
            for b in range(n_part):
                to = n_near - 1 - n if (a - b) % n_part * 2 == n_part else n
                pairs.append(((a * n_near + n) * n_part + b, (b * n_near + to) * n_part + a))
    return lax.ppermute(own, ("part", "near", "col"), pairs)


def gathered_pieces(turned):
    near, core = lax.axis_index("near"), lax.axis_index("core")
    n_part, n_near = lax.axis_size("part"), lax.axis_size("near")
    parts, codes = turned[None], [0]
    bit = n_near // 2
    while bit:
        parts = jnp.concatenate([parts, swap(parts, "near", bit)], axis=0)
        codes = codes + [code ^ bit for code in codes]
        bit //= 2
    other = swap(parts, "core", 1)
    flip = flipped(lax.axis_index("part"), lax.axis_index("col"), n_part, n_near)
    place = ((near ^ flip) * 2 + core).astype(jnp.int32)
    codes = [code * 2 for code in codes] + [code * 2 + 1 for code in codes]
    return parts, other, place, codes


def scattered_sum(value, axis):
    size, at = lax.axis_size(axis), lax.axis_index(axis)
    total = lax.dynamic_index_in_dim(value, at, 0, keepdims=False).astype(f32)
    for k in range(1, size):
        piece = lax.dynamic_index_in_dim(value, (at + k) % size, 0, keepdims=False)
        piece = lax.ppermute(piece, axis, [(n, (n + k) % size) for n in range(size)])
        total = total + piece.astype(f32)
    return total


def on_device(
    pair_grid,
    alignment_pool,
    sample_index,
    token_mask,
    outer_proj,
    outer_mix,
    pair_logit,
    average_proj,
    average_mix,
    triangle_proj,
    triangle_mix,
    transition_up,
    transition_down,
):
    n_row = lax.axis_size(ROW)
    n_col = lax.axis_size("col")
    tok_row = pair_grid.shape[0]
    tok_col = pair_grid.shape[1]
    pair_width = pair_grid.shape[2]
    samples = sample_index.shape[0]
    align_width = alignment_pool.shape[2]
    outer_width = outer_proj.shape[1] // 2
    head_count = pair_logit.shape[1]
    head_total = average_proj.shape[1] // 2
    head_dim = head_total // head_count
    row_start = lax.axis_index(ROW) * tok_row
    column_start = lax.axis_index("col") * tok_col
    quarter = samples // n_col
    sample_start = lax.axis_index("col") * quarter

    norm_t, norm_flat = drawn_alignments(alignment_pool, sample_index)
    turned = turned_rows(norm_flat)

    group = 16
    mix_d = outer_mix.reshape(outer_width, outer_width, pair_width).transpose(1, 0, 2)
    mixed = mixed_rows(norm_t, outer_proj[:, :outer_width], mix_d, group, 4)
    same = jnp.eye(group, dtype=bf16)
    spread = (
        same[None, :, :, None] * outer_proj[:, outer_width:].T[:, None, None, :]
    ).reshape(outer_width * group, group * align_width)
    row_mask = lax.dynamic_slice_in_dim(token_mask, row_start, tok_row, 0).astype(f32)
    column_mask = lax.dynamic_slice_in_dim(token_mask, column_start, tok_col, 0).astype(f32)
    pair_mask = (row_mask[:, None] * column_mask[None, :])[:, None, :]
    proj_t, logit_t = triangle_proj[:, : 4 * pair_width].T, pair_logit.T
    turned, mixed, spread, proj_t, logit_t, pair_mask = lax.optimization_barrier(
        (turned, mixed, spread, proj_t, logit_t, pair_mask)
    )
    parts, other, place, codes = gathered_pieces(turned)
    pair_one, pair_norm, weights, factors = pair_part(
        place.reshape(1), codes, parts, other, spread, mixed, pair_grid, proj_t, logit_t, pair_mask
    )

    factors, parts, other, pool, index = lax.optimization_barrier(
        (factors, parts, other, alignment_pool, sample_index)
    )
    received = lax.all_to_all(factors, ROW_COL, split_axis=0, concat_axis=0, tiled=True)

    value_weight = average_proj[:, :head_total].reshape(align_width, head_count, head_dim)
    gate_weight = average_proj[:, head_total:]
    partial_total = jnp.sum(weights, axis=2)
    low_weights = weights.astype(bf16).reshape(tok_row * head_count, tok_col)
    half = tok_col // 2
    drawn = 0.0
    for n, pieces in enumerate((parts, other)):
        row = lax.broadcasted_iota(jnp.int32, (tok_col, half), 0)
        lane = lax.broadcasted_iota(jnp.int32, (tok_col, half), 1)
        code = jnp.repeat(jnp.array(codes[n * len(codes) // 2 :][: half // tok_row]), tok_row)
        source = (place ^ code[None, :]) * tok_row + lane % tok_row
        pick = jnp.where(row == source, 1.0, 0.0).astype(bf16)
        sorted_weights = jnp.dot(low_weights, pick, preferred_element_type=f32).astype(bf16)
        drawn = drawn + jnp.dot(
            sorted_weights, pieces.reshape(half, samples * align_width),
            preferred_element_type=f32,
        )
    drawn = drawn.astype(bf16).reshape(tok_row, head_count, samples, align_width)
    partial_sum = jnp.einsum(
        "ihsm,mhc->sihc", drawn, value_weight, preferred_element_type=f32
    ).astype(bf16).reshape(n_col, quarter, tok_row, head_total)
    high = partial_total.astype(bf16)
    low = (partial_total - high.astype(f32)).astype(bf16)
    total_row = jnp.concatenate([high, low], axis=1)
    total_row = jnp.pad(total_row, ((0, 0), (0, head_total - 2 * head_count)))
    total_row = jnp.broadcast_to(total_row, (n_col, 1, tok_row, head_total))
    sums = jnp.concatenate([partial_sum, total_row], axis=1)
    sums = scattered_sum(sums, "col")
    received, sums = lax.optimization_barrier((received, sums))
    totals = sums[quarter, :, :head_count] + sums[quarter, :, head_count : 2 * head_count]
    weighted = sums[:quarter]
    own_index = lax.dynamic_slice_in_dim(index, sample_start, quarter, 0)
    own_align = jnp.take(pool, own_index, axis=0, mode="clip")
    own_norm = normalize(own_align, 2).astype(bf16)
    gate_values = jax.nn.sigmoid(
        jnp.einsum("sim,mk->sik", own_norm, gate_weight, preferred_element_type=f32)
    )
    share = jnp.repeat(1.0 / totals, head_dim, axis=1)
    averaged = (gate_values * weighted * share).astype(bf16)
    align_update = jnp.einsum("sik,km->sim", averaged, average_mix, preferred_element_type=f32)
    own_next = (own_align.astype(f32) + align_update).astype(bf16)
    alignment_next = lax.all_gather(own_next, "col", axis=0, tiled=True)

    result = triangle(received.reshape(n_row, n_col, 2, tok_row, tok_col))
    product = lax.all_to_all(
        result.reshape(n_row * n_col, tok_row, tok_col), ROW_COL,
        split_axis=0, concat_axis=0, tiled=True,
    )
    flat_norm = pair_norm.reshape(tok_row * tok_col, pair_width)
    gate_out = jax.nn.sigmoid(
        jnp.dot(flat_norm, triangle_proj[:, 4 * pair_width :], preferred_element_type=f32)
    ).reshape(pair_grid.shape)
    return tuple(
        tail(
            product, pair_one, gate_out, triangle_mix, transition_up, transition_down,
            alignment_next,
        )
    )


def solution(mesh):
    n_groups, n_row, n_col = mesh.shape["groups"], mesh.shape["row"], mesh.shape["col"]
    split = Mesh(
        mesh.devices.reshape(n_groups, n_col, n_row // n_col // 2, 2, n_col),
        ("groups", "part", "near", "core", "col"),
    )
    placed = (
        P(GROUPS_ROW, "col", None),
        P("groups", ROW, None),
        P("groups"),
        P("groups"),
    ) + (P(),) * 9
    return jax.shard_map(
        on_device,
        mesh=split,
        in_specs=placed,
        out_specs=(P(GROUPS_ROW, "col", None), P("groups", ROW, None)),
        check_vma=False,
    )
```

```python
import functools

import jax
import jax.numpy as jnp
from jax import lax
from jax.experimental import pallas as pl
from jax.experimental.pallas import tpu as pltpu
from jax.sharding import Mesh
from jax.sharding import PartitionSpec as P

ROW = ("part", "near", "core")
ROW_COL = ("part", "near", "core", "col")
GROUPS_ROW = ("groups", "part", "near", "core")

epsilon = 1e-05
f32 = jnp.float32
bf16 = jnp.bfloat16
NT = (((1,), (1,)), ((), ()))
TN = (((0,), (0,)), ((), ()))


def normalize(values, channel_dim):
    values = values.astype(f32)
    centred = values - jnp.mean(values, axis=channel_dim, keepdims=True)
    spread = jnp.mean(centred * centred, axis=channel_dim, keepdims=True)
    return centred * lax.rsqrt(spread + epsilon)


def sigmoid(x):
    return 1.0 / (1.0 + jnp.exp(-x))


def whole(shape):
    return pl.BlockSpec(shape, lambda *_: (0,) * len(shape))


def draw_kernel(index_ref, pool_ref, turn_ref, flat_ref, normed_ref):
    tokens, samples, width = turn_ref.shape
    stored = pool_ref.shape[2]
    at = lax.broadcasted_iota(jnp.int32, (stored, samples), 0)
    pick = jnp.where(at == index_ref[...], 1.0, 0.0).astype(f32).T.astype(bf16)
    for t in range(tokens):
        drawn = lax.dot_general(pick, pool_ref[t], NT, preferred_element_type=f32)
        normed = normalize(drawn, 1)
        turn_ref[t] = normed.astype(bf16)
        normed_ref[t * samples : (t + 1) * samples, :] = normed
    for s in range(0, samples, 2):
        both = jnp.concatenate(
            [normed_ref[pl.ds(s + n, tokens, stride=samples), :] for n in range(2)], axis=1
        )
        flat_ref[:, s * width : (s + 2) * width] = both.astype(bf16)


def drawn_alignments(pool, index):
    _, tokens, width = pool.shape
    samples = index.shape[0]
    vmem = pl.BlockSpec(memory_space=pltpu.VMEM)
    return pl.pallas_call(
        draw_kernel,
        in_specs=[vmem] * 2,
        out_specs=[vmem] * 2,
        out_shape=[
            jax.ShapeDtypeStruct((tokens, samples, width), bf16),
            jax.ShapeDtypeStruct((tokens, samples * width), bf16),
        ],
        scratch_shapes=[pltpu.VMEM((tokens * samples, width), f32)],
        name="draw",
    )(index.reshape(1, samples), pool.transpose(1, 2, 0))


def mix_kernel(
    norm_ref, proj_ref, mix_ref, mixed_ref, spread_ref,
    rows_ref, wide_ref, pairs_ref, held_ref, sem, *, scale,
):
    step = pl.program_id(0)
    tokens, samples, align = norm_ref.shape
    inner = rows_ref.shape[1]
    depth, width = pairs_ref.shape[0] * 2, mix_ref.shape[1]
    groups, group = held_ref.shape[1], held_ref.shape[3]
    rows = held_ref.shape[4] // width

    @pl.when(step == 0)
    def _():
        flat = norm_ref[...].reshape(tokens * samples, align)
        both = jnp.dot(flat, proj_ref[...], preferred_element_type=f32)
        rows_ref[...] = both[:, :inner].astype(bf16)
        wide_ref[...] = mix_ref[...].astype(f32)
        for d in range(depth):
            picked = wide_ref[pl.ds(d, inner, stride=depth), :].astype(bf16)
            pairs_ref[d // 2, :, (d % 2) * width : (d % 2 + 1) * width] = picked
        turned = proj_ref[...].astype(f32).T[inner:]
        turned = jnp.concatenate([turned, turned], axis=1)
        turned = jnp.broadcast_to(turned[:, None, :], (depth, group, 2 * align))
        turned = turned.reshape(depth * group, 2 * align)
        row = lax.broadcasted_iota(jnp.int32, turned.shape, 0) % group
        lane = lax.broadcasted_iota(jnp.int32, turned.shape, 1) // align
        for s in range(0, group, 2):
            chunk = jnp.where(row == lane + s, turned, 0.0)
            spread_ref[:, s * align : (s + 2) * align] = chunk.astype(bf16)

    block = rows_ref[pl.ds(pl.multiple_of(step * rows * samples, samples), rows * samples), :]
    for d in range(depth):
        if d % 2 == 0:
            part = jnp.dot(block, pairs_ref[d // 2], preferred_element_type=f32) * scale
            part = part.astype(bf16)
        for i in range(rows):
            for g in range(groups):
                at = i * samples + g * group
                held_ref[step, g, d, :, i * width : (i + 1) * width] = part[
                    at : at + group, (d % 2) * width : (d % 2 + 1) * width
                ]

    def copy(n, g):
        return pltpu.make_async_copy(held_ref.at[n, g], mixed_ref.at[n, g], sem.at[n, g])

    for g in range(groups):
        copy(step, g).start()

    @pl.when(step == pl.num_programs(0) - 1)
    def _():
        for n in range(tokens // rows):
            for g in range(groups):
                copy(n, g).wait()


def mixed_rows(norm_t, proj, mix, group, rows):
    tokens, samples, align = norm_t.shape
    width = mix.shape[1]
    depth = proj.shape[1] // 2
    inner = mix.shape[0] // depth
    steps = tokens // rows
    shape = (steps, samples // group, depth, group, rows * width)
    mixed, spread = pl.pallas_call(
        functools.partial(mix_kernel, scale=1.0 / samples),
        grid=(steps,),
        in_specs=[whole(norm_t.shape), whole(proj.shape), whole(mix.shape)],
        out_specs=[pl.BlockSpec(memory_space=pl.ANY), whole((depth * group, group * align))],
        out_shape=[
            jax.ShapeDtypeStruct(shape, bf16),
            jax.ShapeDtypeStruct((depth * group, group * align), bf16),
        ],
        scratch_shapes=[
            pltpu.VMEM((tokens * samples, inner), bf16),
            pltpu.VMEM(mix.shape, f32),
            pltpu.VMEM((depth // 2, inner, 2 * width), bf16),
            pltpu.VMEM(shape, bf16),
            pltpu.SemaphoreType.DMA(shape[:2]),
        ],
        cost_estimate=pl.CostEstimate(
            flops=16 * tokens * samples * inner * depth * width,
            bytes_accessed=2 * tokens * samples * depth * width,
            transcendentals=0,
        ),
        name="mixed_rows",
    )(norm_t, proj, mix)
    return mixed.reshape(steps, samples // group, depth * group, rows * width), spread


def pair_kernel(
    place_ref, first_ref, side_ref, token_ref,
    own_ref, other_ref, spread_ref, mixed_ref, pair_ref, proj_ref, logit_ref, mask_ref,
    one_ref, pnorm_ref, weight_ref, factor_ref,
    held_ref, col_ref, proj_t_ref, left_ref, right_ref, made_ref, sem, out_sem, *, codes,
):
    step = pl.program_id(0)
    rows, cols, width = pair_ref.shape
    tokens = made_ref.shape[2]
    got, chunk = spread_ref.shape
    kept = own_ref.shape[0]
    blocks, groups = mixed_ref.shape[0], mixed_ref.shape[1]

    def fetch(n, g):
        return pltpu.make_async_copy(
            mixed_ref.at[n, g], held_ref.at[n, pl.ds(g * got, got)], sem.at[n, g]
        )

    @pl.when(step == 0)
    def _():
        for n in range(blocks):
            for g in range(groups):
                fetch(n, g).start()
        proj_t_ref[...] = proj_ref[:, : 4 * width].astype(f32).T.astype(bf16)
        block = jnp.concatenate(
            [ref[...].reshape(kept * tokens, ref.shape[2]) for ref in (own_ref, other_ref)], axis=0
        )
        for g in range(block.shape[1] // chunk):
            part = lax.dot_general(
                block[:, g * chunk : (g + 1) * chunk], spread_ref[...], NT,
                preferred_element_type=f32,
            ).astype(bf16)
            for n, code in enumerate(codes):
                at = pl.multiple_of((place_ref[0] ^ code) * tokens, tokens)
                col_ref[pl.ds(at, tokens), g * got : (g + 1) * got] = part[
                    n * tokens : (n + 1) * tokens
                ]

    for g in range(groups):
        fetch(step, g).wait()
    update = jnp.dot(col_ref[...], held_ref[step], preferred_element_type=f32)
    normed = []
    for n in range(rows):
        one = (pair_ref[n].astype(f32) + update[:, n * width : (n + 1) * width]).astype(bf16)
        one_ref[n] = one
        now = normalize(one, 1).astype(bf16)
        pnorm_ref[n] = now
        normed.append(now)
    normed = jnp.concatenate(normed, axis=0)
    projected = lax.dot_general(proj_t_ref[...], normed, NT, preferred_element_type=f32)
    scores = jnp.exp(lax.dot_general(logit_ref[...], normed, NT, preferred_element_type=f32))
    left = sigmoid(projected[:width]) * projected[width : 2 * width]
    right = sigmoid(projected[2 * width : 3 * width]) * projected[3 * width :]
    column_mask = mask_ref[pl.ds(side_ref[0], 1), :].astype(f32)
    for n in range(rows):
        weight_ref[n] = scores[:, n * cols : (n + 1) * cols]
        mask = column_mask * token_ref[first_ref[0] + step * rows + n].astype(f32)
        lanes = slice(n * cols, (n + 1) * cols)
        at = pl.ds(step * rows + n, width, stride=tokens)
        left_ref[at, :] = left[:, lanes] * mask
        right_ref[at, :] = right[:, lanes] * mask

    @pl.when(step == pl.num_programs(0) - 1)
    def _():
        sends = out_sem.shape[0]
        share = width // sends
        copies = []
        for n in range(sends):
            own = slice(n * share, (n + 1) * share)
            for side, ref in enumerate((left_ref, right_ref)):
                block = ref[n * share * tokens : (n + 1) * share * tokens, :]
                made_ref[own, side] = block.reshape(share, tokens, cols).astype(bf16)
            copy = pltpu.make_async_copy(
                made_ref.at[pl.ds(n * share, share)], factor_ref.at[pl.ds(n * share, share)],
                out_sem.at[n],
            )
            copy.start()
            copies.append(copy)
        for copy in copies:
            copy.wait()


def pair_part(scalars, codes, own, other, spread, mixed, pair_grid, proj, logit_t, mask):
    tokens, cols, width = pair_grid.shape
    heads = logit_t.shape[0]
    steps, groups, got, wide = mixed.shape
    rows = wide // width
    depth = groups * got
    pairs = pl.BlockSpec((rows, cols, width), lambda n, *_: (n, 0, 0))
    anywhere = pl.BlockSpec(memory_space=pl.ANY)
    return pl.pallas_call(
        functools.partial(pair_kernel, codes=codes),
        grid_spec=pltpu.PrefetchScalarGridSpec(
            num_scalar_prefetch=4,
            grid=(steps,),
            in_specs=[
                whole(own.shape),
                whole(other.shape),
                whole(spread.shape),
                anywhere,
                pairs,
                whole(proj.shape),
                whole(logit_t.shape),
                whole(mask.shape),
            ],
            out_specs=[
                pairs,
                pairs,
                pl.BlockSpec((rows, heads, cols), lambda n, *_: (n, 0, 0)),
                anywhere,
            ],
            scratch_shapes=[
                pltpu.VMEM((steps, depth, wide), bf16),
                pltpu.VMEM((cols, depth), bf16),
                pltpu.VMEM((4 * width, width), bf16),
                pltpu.VMEM((width * tokens, cols), f32),
                pltpu.VMEM((width * tokens, cols), f32),
                pltpu.VMEM((width, 2, tokens, cols), bf16),
                pltpu.SemaphoreType.DMA((steps, groups)),
                pltpu.SemaphoreType.DMA((8,)),
            ],
        ),
        out_shape=[
            jax.ShapeDtypeStruct(pair_grid.shape, bf16),
            jax.ShapeDtypeStruct(pair_grid.shape, bf16),
            jax.ShapeDtypeStruct((tokens, heads, cols), f32),
            jax.ShapeDtypeStruct((width, 2, tokens, cols), bf16),
        ],
        name="pair_part",
    )(*scalars, own, other, spread, mixed, pair_grid, proj, logit_t, mask)


def triangle_kernel(got_ref, out_ref):
    n_row, n_col, _, tokens, cols = got_ref.shape
    sides = []
    for side in range(2):
        sides.append(
            jnp.concatenate(
                [got_ref[:, x, side].reshape(n_row * tokens, cols) for x in range(n_col)], axis=1
            )
        )
    product = lax.dot_general(sides[0], sides[1], NT, preferred_element_type=f32).astype(bf16)
    for x in range(n_col):
        out_ref[:, x] = product[:, x * cols : (x + 1) * cols].reshape(n_row, tokens, cols)


def triangle(got):
    n_row, n_col, _, tokens, cols = got.shape
    return pl.pallas_call(
        triangle_kernel,
        out_shape=jax.ShapeDtypeStruct((n_row, n_col, tokens, cols), bf16),
        in_specs=[pl.BlockSpec(memory_space=pltpu.VMEM)],
        out_specs=pl.BlockSpec(memory_space=pltpu.VMEM),
        compiler_params=pltpu.CompilerParams(vmem_limit_bytes=16 * 1024 * 1024),
        name="triangle",
    )(got)


def tail_kernel(
    product_ref, one_ref, gate_ref, mix_ref, up_ref, down_ref, next_ref,
    out_ref, copied_ref, turned_ref,
):
    step = pl.program_id(0)
    rows, cols, width = one_ref.shape
    _, tokens, _ = product_ref.shape
    inner = down_ref.shape[0]

    @pl.when(step == 0)
    def _():
        turned_ref[...] = normalize(product_ref[...], 0).reshape(width * tokens, cols)
        copied_ref[...] = next_ref[...]

    pair_two = []
    for n in range(rows):
        block = turned_ref[pl.ds(step * rows + n, width, stride=tokens), :].astype(bf16)
        mixed = lax.dot_general(block, mix_ref[...], TN, preferred_element_type=f32)
        pair_two.append((one_ref[n].astype(f32) + gate_ref[n] * mixed).astype(bf16))
    pair_two = jnp.concatenate(pair_two, axis=0)
    normed = normalize(pair_two, 1).astype(bf16)
    first = jnp.dot(normed, up_ref[:, :inner], preferred_element_type=f32)
    second = jnp.dot(normed, up_ref[:, inner:], preferred_element_type=f32)
    hidden = (first * sigmoid(first) * second).astype(bf16)
    update = jnp.dot(hidden, down_ref[...], preferred_element_type=f32)
    out_ref[...] = (pair_two.astype(f32) + update).astype(bf16).reshape(rows, cols, width)


def tail(product, one, gate, mix, up, down, following):
    tokens, cols, width = one.shape
    rows = 4
    pairs = pl.BlockSpec((rows, cols, width), lambda n: (n, 0, 0))
    return pl.pallas_call(
        tail_kernel,
        grid=(tokens // rows,),
        in_specs=[
            whole(product.shape), pairs, pairs, whole(mix.shape), whole(up.shape),
            whole(down.shape), whole(following.shape),
        ],
        out_specs=[pairs, whole(following.shape)],
        out_shape=[
            jax.ShapeDtypeStruct(one.shape, bf16),
            jax.ShapeDtypeStruct(following.shape, bf16),
        ],
        scratch_shapes=[pltpu.VMEM((width * tokens, cols), f32)],
        compiler_params=pltpu.CompilerParams(vmem_limit_bytes=24 * 1024 * 1024),
        name="tail",
    )(product, one, gate, mix, up, down, following)


def swap(value, axis, bit):
    size = lax.axis_size(axis)
    return lax.ppermute(value, axis, [(n, n ^ bit) for n in range(size)])


def flipped(part, col, n_part, n_near):
    return jnp.where((part - col) % n_part * 2 == n_part, n_near - 1, 0)


def turned_rows(own):
    n_part, n_near = lax.axis_size("part"), lax.axis_size("near")
    pairs = []
    for a in range(n_part):
        for n in range(n_near):
            for b in range(n_part):
                to = n_near - 1 - n if (a - b) % n_part * 2 == n_part else n
                pairs.append(((a * n_near + n) * n_part + b, (b * n_near + to) * n_part + a))
    return lax.ppermute(own, ("part", "near", "col"), pairs)


def gathered_pieces(turned):
    near, core = lax.axis_index("near"), lax.axis_index("core")
    n_part, n_near = lax.axis_size("part"), lax.axis_size("near")
    parts, codes = turned[None], [0]
    bit = n_near // 2
    while bit:
        parts = jnp.concatenate([parts, swap(parts, "near", bit)], axis=0)
        codes = codes + [code ^ bit for code in codes]
        bit //= 2
    other = swap(parts, "core", 1)
    flip = flipped(lax.axis_index("part"), lax.axis_index("col"), n_part, n_near)
    place = ((near ^ flip) * 2 + core).astype(jnp.int32)
    codes = [code * 2 for code in codes] + [code * 2 + 1 for code in codes]
    return parts, other, place, codes


def scattered_sum(value, axis):
    size, at = lax.axis_size(axis), lax.axis_index(axis)
    total = lax.dynamic_index_in_dim(value, at, 0, keepdims=False).astype(f32)
    for k in range(1, size):
        piece = lax.dynamic_index_in_dim(value, (at + k) % size, 0, keepdims=False)
        piece = lax.ppermute(piece, axis, [(n, (n + k) % size) for n in range(size)])
        total = total + piece.astype(f32)
    return total


def on_device(
    pair_grid,
    alignment_pool,
    sample_index,
    token_mask,
    outer_proj,
    outer_mix,
    pair_logit,
    average_proj,
    average_mix,
    triangle_proj,
    triangle_mix,
    transition_up,
    transition_down,
):
    n_row = lax.axis_size(ROW)
    n_col = lax.axis_size("col")
    tok_row = pair_grid.shape[0]
    tok_col = pair_grid.shape[1]
    pair_width = pair_grid.shape[2]
    samples = sample_index.shape[0]
    align_width = alignment_pool.shape[2]
    head_count = pair_logit.shape[1]
    head_total = average_proj.shape[1] // 2
    head_dim = head_total // head_count
    quarter = samples // n_col
    sample_start = lax.axis_index("col") * quarter

    norm_t, norm_flat = drawn_alignments(alignment_pool, sample_index)
    turned = turned_rows(norm_flat)

    mixed, spread = mixed_rows(norm_t, outer_proj, outer_mix, 16, 4)
    turned, mixed, spread = lax.optimization_barrier((turned, mixed, spread))
    parts, other, place, codes = gathered_pieces(turned)
    row_start = lax.axis_index(ROW) * tok_row
    scalars = [
        value.astype(jnp.int32).reshape(1) for value in (place, row_start, lax.axis_index("col"))
    ]
    pair_one, pair_norm, weights, factors = pair_part(
        scalars + [token_mask], codes, parts, other, spread, mixed, pair_grid, triangle_proj,
        pair_logit.T, token_mask.reshape(n_col, tok_col),
    )

    factors, parts, other, pool, index = lax.optimization_barrier(
        (factors, parts, other, alignment_pool, sample_index)
    )
    received = lax.all_to_all(factors, ROW_COL, split_axis=0, concat_axis=0, tiled=True)

    value_weight = average_proj[:, :head_total].reshape(align_width, head_count, head_dim)
    gate_weight = average_proj[:, head_total:]
    partial_total = jnp.sum(weights, axis=2)
    low_weights = weights.astype(bf16).reshape(tok_row * head_count, tok_col)
    half = tok_col // 2
    drawn = 0.0
    for n, pieces in enumerate((parts, other)):
        row = lax.broadcasted_iota(jnp.int32, (tok_col, half), 0)
        lane = lax.broadcasted_iota(jnp.int32, (tok_col, half), 1)
        code = jnp.repeat(jnp.array(codes[n * len(codes) // 2 :][: half // tok_row]), tok_row)
        source = (place ^ code[None, :]) * tok_row + lane % tok_row
        pick = jnp.where(row == source, 1.0, 0.0).astype(bf16)
        sorted_weights = jnp.dot(low_weights, pick, preferred_element_type=f32).astype(bf16)
        drawn = drawn + jnp.dot(
            sorted_weights, pieces.reshape(half, samples * align_width),
            preferred_element_type=f32,
        )
    drawn = drawn.astype(bf16).reshape(tok_row, head_count, samples, align_width)
    partial_sum = jnp.einsum(
        "ihsm,mhc->sihc", drawn, value_weight, preferred_element_type=f32
    ).astype(bf16).reshape(n_col, quarter, tok_row, head_total)
    high = partial_total.astype(bf16)
    low = (partial_total - high.astype(f32)).astype(bf16)
    total_row = jnp.concatenate([high, low], axis=1)
    total_row = jnp.pad(total_row, ((0, 0), (0, head_total - 2 * head_count)))
    total_row = jnp.broadcast_to(total_row, (n_col, 1, tok_row, head_total))
    sums = jnp.concatenate([partial_sum, total_row], axis=1)
    sums = scattered_sum(sums, "col")
    received, sums = lax.optimization_barrier((received, sums))
    totals = sums[quarter, :, :head_count] + sums[quarter, :, head_count : 2 * head_count]
    weighted = sums[:quarter]
    own_index = lax.dynamic_slice_in_dim(index, sample_start, quarter, 0)
    own_align = jnp.take(pool, own_index, axis=0, mode="clip")
    own_norm = normalize(own_align, 2).astype(bf16)
    gate_values = jax.nn.sigmoid(
        jnp.einsum("sim,mk->sik", own_norm, gate_weight, preferred_element_type=f32)
    )
    share = jnp.repeat(1.0 / totals, head_dim, axis=1)
    averaged = (gate_values * weighted * share).astype(bf16)
    align_update = jnp.einsum("sik,km->sim", averaged, average_mix, preferred_element_type=f32)
    own_next = (own_align.astype(f32) + align_update).astype(bf16)
    alignment_next = lax.all_gather(own_next, "col", axis=0, tiled=True)

    result = triangle(received.reshape(n_row, n_col, 2, tok_row, tok_col))
    product = lax.all_to_all(
        result.reshape(n_row * n_col, tok_row, tok_col), ROW_COL,
        split_axis=0, concat_axis=0, tiled=True,
    )
    flat_norm = pair_norm.reshape(tok_row * tok_col, pair_width)
    gate_out = jax.nn.sigmoid(
        jnp.dot(flat_norm, triangle_proj[:, 4 * pair_width :], preferred_element_type=f32)
    ).reshape(pair_grid.shape)
    return tuple(
        tail(
            product, pair_one, gate_out, triangle_mix, transition_up, transition_down,
            alignment_next,
        )
    )


def solution(mesh):
    n_groups, n_row, n_col = mesh.shape["groups"], mesh.shape["row"], mesh.shape["col"]
    split = Mesh(
        mesh.devices.reshape(n_groups, n_col, n_row // n_col // 2, 2, n_col),
        ("groups", "part", "near", "core", "col"),
    )
    placed = (
        P(GROUPS_ROW, "col", None),
        P("groups", ROW, None),
        P("groups"),
        P("groups"),
    ) + (P(),) * 9
    return jax.shard_map(
        on_device,
        mesh=split,
        in_specs=placed,
        out_specs=(P(GROUPS_ROW, "col", None), P("groups", ROW, None)),
        check_vma=False,
    )
```

```python
import functools

import jax
import jax.numpy as jnp
from jax import lax
from jax.experimental import pallas as pl
from jax.experimental.pallas import tpu as pltpu
from jax.sharding import Mesh
from jax.sharding import PartitionSpec as P

ROW = ("part", "near", "core")
ROW_COL = ("part", "near", "core", "col")
GROUPS_ROW = ("groups", "part", "near", "core")

epsilon = 1e-05
f32 = jnp.float32
bf16 = jnp.bfloat16
NT = (((1,), (1,)), ((), ()))
TN = (((0,), (0,)), ((), ()))


def normalize(values, channel_dim):
    values = values.astype(f32)
    centred = values - jnp.mean(values, axis=channel_dim, keepdims=True)
    spread = jnp.mean(centred * centred, axis=channel_dim, keepdims=True)
    return centred * lax.rsqrt(spread + epsilon)


def sigmoid(x):
    return 1.0 / (1.0 + jnp.exp(-x))


def whole(shape):
    return pl.BlockSpec(shape, lambda *_: (0,) * len(shape))


def draw_kernel(index_ref, pool_ref, turn_ref, flat_ref, normed_ref):
    tokens, samples, width = turn_ref.shape
    stored = pool_ref.shape[2]
    at = lax.broadcasted_iota(jnp.int32, (stored, samples), 0)
    pick = jnp.where(at == index_ref[...], 1.0, 0.0).astype(f32).T.astype(bf16)
    for t in range(tokens):
        drawn = lax.dot_general(pick, pool_ref[t], NT, preferred_element_type=f32)
        normed = normalize(drawn, 1)
        turn_ref[t] = normed.astype(bf16)
        normed_ref[t * samples : (t + 1) * samples, :] = normed
    for s in range(0, samples, 2):
        both = jnp.concatenate(
            [normed_ref[pl.ds(s + n, tokens, stride=samples), :] for n in range(2)], axis=1
        )
        flat_ref[:, s * width : (s + 2) * width] = both.astype(bf16)


def drawn_alignments(pool, index):
    _, tokens, width = pool.shape
    samples = index.shape[0]
    vmem = pl.BlockSpec(memory_space=pltpu.VMEM)
    return pl.pallas_call(
        draw_kernel,
        in_specs=[vmem] * 2,
        out_specs=[vmem] * 2,
        out_shape=[
            jax.ShapeDtypeStruct((tokens, samples, width), bf16),
            jax.ShapeDtypeStruct((tokens, samples * width), bf16),
        ],
        scratch_shapes=[pltpu.VMEM((tokens * samples, width), f32)],
        name="draw",
    )(index.reshape(1, samples), pool.transpose(1, 2, 0))


def mix_kernel(
    norm_ref, proj_ref, mix_ref, mixed_ref, spread_ref,
    rows_ref, wide_ref, pairs_ref, held_ref, sem, *, scale,
):
    step = pl.program_id(0)
    tokens, samples, align = norm_ref.shape
    inner = rows_ref.shape[1]
    depth, width = pairs_ref.shape[0] * 2, mix_ref.shape[1]
    groups, group = held_ref.shape[1], held_ref.shape[3]
    rows = held_ref.shape[4] // width

    @pl.when(step == 0)
    def _():
        flat = norm_ref[...].reshape(tokens * samples, align)
        both = jnp.dot(flat, proj_ref[...], preferred_element_type=f32)
        rows_ref[...] = both[:, :inner].astype(bf16)
        wide_ref[...] = mix_ref[...].astype(f32)
        for d in range(depth):
            picked = wide_ref[pl.ds(d, inner, stride=depth), :].astype(bf16)
            pairs_ref[d // 2, :, (d % 2) * width : (d % 2 + 1) * width] = picked
        turned = proj_ref[...].astype(f32).T[inner:]
        turned = jnp.concatenate([turned, turned], axis=1)
        turned = jnp.broadcast_to(turned[:, None, :], (depth, group, 2 * align))
        turned = turned.reshape(depth * group, 2 * align)
        row = lax.broadcasted_iota(jnp.int32, turned.shape, 0) % group
        lane = lax.broadcasted_iota(jnp.int32, turned.shape, 1) // align
        for s in range(0, group, 2):
            chunk = jnp.where(row == lane + s, turned, 0.0)
            spread_ref[:, s * align : (s + 2) * align] = chunk.astype(bf16)

    block = rows_ref[pl.ds(pl.multiple_of(step * rows * samples, samples), rows * samples), :]
    for d in range(depth):
        if d % 2 == 0:
            part = jnp.dot(block, pairs_ref[d // 2], preferred_element_type=f32) * scale
            part = part.astype(bf16)
        for i in range(rows):
            for g in range(groups):
                at = i * samples + g * group
                held_ref[step, g, d, :, i * width : (i + 1) * width] = part[
                    at : at + group, (d % 2) * width : (d % 2 + 1) * width
                ]

    def copy(n, g):
        return pltpu.make_async_copy(held_ref.at[n, g], mixed_ref.at[n, g], sem.at[n, g])

    for g in range(groups):
        copy(step, g).start()

    @pl.when(step == pl.num_programs(0) - 1)
    def _():
        for n in range(tokens // rows):
            for g in range(groups):
                copy(n, g).wait()


def mixed_rows(norm_t, proj, mix, group, rows):
    tokens, samples, align = norm_t.shape
    width = mix.shape[1]
    depth = proj.shape[1] // 2
    inner = mix.shape[0] // depth
    steps = tokens // rows
    shape = (steps, samples // group, depth, group, rows * width)
    mixed, spread = pl.pallas_call(
        functools.partial(mix_kernel, scale=1.0 / samples),
        grid=(steps,),
        in_specs=[whole(norm_t.shape), whole(proj.shape), whole(mix.shape)],
        out_specs=[pl.BlockSpec(memory_space=pltpu.HBM), whole((depth * group, group * align))],
        out_shape=[
            jax.ShapeDtypeStruct(shape, bf16),
            jax.ShapeDtypeStruct((depth * group, group * align), bf16),
        ],
        scratch_shapes=[
            pltpu.VMEM((tokens * samples, inner), bf16),
            pltpu.VMEM(mix.shape, f32),
            pltpu.VMEM((depth // 2, inner, 2 * width), bf16),
            pltpu.VMEM(shape, bf16),
            pltpu.SemaphoreType.DMA(shape[:2]),
        ],
        cost_estimate=pl.CostEstimate(
            flops=16 * tokens * samples * inner * depth * width,
            bytes_accessed=2 * tokens * samples * depth * width,
            transcendentals=0,
        ),
        name="mixed_rows",
    )(norm_t, proj, mix)
    return mixed.reshape(steps, samples // group, depth * group, rows * width), spread


def pair_kernel(
    place_ref, first_ref, side_ref, token_ref,
    own_ref, other_ref, spread_ref, mixed_ref, pair_ref, proj_ref, logit_ref, mask_ref,
    one_ref, pnorm_ref, weight_ref, factor_ref,
    held_ref, col_ref, proj_t_ref, left_ref, right_ref, made_ref, sem, out_sem, *, codes,
):
    step = pl.program_id(0)
    rows, cols, width = pair_ref.shape
    tokens = made_ref.shape[2]
    got, chunk = spread_ref.shape
    kept = own_ref.shape[0]
    blocks, groups = mixed_ref.shape[0], mixed_ref.shape[1]

    def fetch(n, g):
        return pltpu.make_async_copy(
            mixed_ref.at[n, g], held_ref.at[n, pl.ds(g * got, got)], sem.at[n, g]
        )

    @pl.when(step == 0)
    def _():
        for g in range(groups):
            fetch(0, g).start()
        proj_t_ref[...] = proj_ref[:, : 4 * width].astype(f32).T.astype(bf16)
        block = jnp.concatenate(
            [ref[...].reshape(kept * tokens, ref.shape[2]) for ref in (own_ref, other_ref)], axis=0
        )
        for g in range(block.shape[1] // chunk):
            part = lax.dot_general(
                block[:, g * chunk : (g + 1) * chunk], spread_ref[...], NT,
                preferred_element_type=f32,
            ).astype(bf16)
            for n, code in enumerate(codes):
                at = pl.multiple_of((place_ref[0] ^ code) * tokens, tokens)
                col_ref[pl.ds(at, tokens), g * got : (g + 1) * got] = part[
                    n * tokens : (n + 1) * tokens
                ]

    @pl.when(step + 1 < blocks)
    def _():
        for g in range(groups):
            fetch(step + 1, g).start()

    for g in range(groups):
        fetch(step, g).wait()
    update = jnp.dot(col_ref[...], held_ref[step], preferred_element_type=f32)
    normed = []
    for n in range(rows):
        one = (pair_ref[n].astype(f32) + update[:, n * width : (n + 1) * width]).astype(bf16)
        one_ref[n] = one
        now = normalize(one, 1).astype(bf16)
        pnorm_ref[n] = now
        normed.append(now)
    normed = jnp.concatenate(normed, axis=0)
    projected = lax.dot_general(proj_t_ref[...], normed, NT, preferred_element_type=f32)
    scores = jnp.exp(lax.dot_general(logit_ref[...], normed, NT, preferred_element_type=f32))
    left = sigmoid(projected[:width]) * projected[width : 2 * width]
    right = sigmoid(projected[2 * width : 3 * width]) * projected[3 * width :]
    column_mask = mask_ref[pl.ds(side_ref[0], 1), :].astype(f32)
    for n in range(rows):
        weight_ref[n] = scores[:, n * cols : (n + 1) * cols]
        mask = column_mask * token_ref[first_ref[0] + step * rows + n].astype(f32)
        lanes = slice(n * cols, (n + 1) * cols)
        at = pl.ds(step * rows + n, width, stride=tokens)
        left_ref[at, :] = left[:, lanes] * mask
        right_ref[at, :] = right[:, lanes] * mask

    @pl.when(step == pl.num_programs(0) - 1)
    def _():
        sends = out_sem.shape[0]
        share = width // sends
        copies = []
        for n in range(sends):
            own = slice(n * share, (n + 1) * share)
            for side, ref in enumerate((left_ref, right_ref)):
                block = ref[n * share * tokens : (n + 1) * share * tokens, :]
                made_ref[own, side] = block.reshape(share, tokens, cols).astype(bf16)
            copy = pltpu.make_async_copy(
                made_ref.at[pl.ds(n * share, share)], factor_ref.at[pl.ds(n * share, share)],
                out_sem.at[n],
            )
            copy.start()
            copies.append(copy)
        for copy in copies:
            copy.wait()


def pair_part(scalars, codes, own, other, spread, mixed, pair_grid, proj, logit_t, mask):
    tokens, cols, width = pair_grid.shape
    heads = logit_t.shape[0]
    steps, groups, got, wide = mixed.shape
    rows = wide // width
    depth = groups * got
    pairs = pl.BlockSpec((rows, cols, width), lambda n, *_: (n, 0, 0))
    anywhere = pl.BlockSpec(memory_space=pltpu.HBM)
    return pl.pallas_call(
        functools.partial(pair_kernel, codes=codes),
        grid_spec=pltpu.PrefetchScalarGridSpec(
            num_scalar_prefetch=4,
            grid=(steps,),
            in_specs=[
                whole(own.shape),
                whole(other.shape),
                whole(spread.shape),
                anywhere,
                pairs,
                whole(proj.shape),
                whole(logit_t.shape),
                whole(mask.shape),
            ],
            out_specs=[
                pairs,
                pairs,
                pl.BlockSpec((rows, heads, cols), lambda n, *_: (n, 0, 0)),
                anywhere,
            ],
            scratch_shapes=[
                pltpu.VMEM((steps, depth, wide), bf16),
                pltpu.VMEM((cols, depth), bf16),
                pltpu.VMEM((4 * width, width), bf16),
                pltpu.VMEM((width * tokens, cols), f32),
                pltpu.VMEM((width * tokens, cols), f32),
                pltpu.VMEM((width, 2, tokens, cols), bf16),
                pltpu.SemaphoreType.DMA((steps, groups)),
                pltpu.SemaphoreType.DMA((8,)),
            ],
        ),
        out_shape=[
            jax.ShapeDtypeStruct(pair_grid.shape, bf16),
            jax.ShapeDtypeStruct(pair_grid.shape, bf16),
            jax.ShapeDtypeStruct((tokens, heads, cols), f32),
            jax.ShapeDtypeStruct((width, 2, tokens, cols), bf16),
        ],
        compiler_params=pltpu.CompilerParams(vmem_limit_bytes=54 * 1024 * 1024),
        name="pair_part",
    )(*scalars, own, other, spread, mixed, pair_grid, proj, logit_t, mask)


def triangle_kernel(got_ref, out_ref):
    n_row, n_col, _, tokens, cols = got_ref.shape
    sides = []
    for side in range(2):
        sides.append(
            jnp.concatenate(
                [got_ref[:, x, side].reshape(n_row * tokens, cols) for x in range(n_col)], axis=1
            )
        )
    product = lax.dot_general(sides[0], sides[1], NT, preferred_element_type=f32).astype(bf16)
    for x in range(n_col):
        out_ref[:, x] = product[:, x * cols : (x + 1) * cols].reshape(n_row, tokens, cols)


def triangle(got):
    n_row, n_col, _, tokens, cols = got.shape
    return pl.pallas_call(
        triangle_kernel,
        out_shape=jax.ShapeDtypeStruct((n_row, n_col, tokens, cols), bf16),
        in_specs=[pl.BlockSpec(memory_space=pltpu.VMEM)],
        out_specs=pl.BlockSpec(memory_space=pltpu.VMEM),
        compiler_params=pltpu.CompilerParams(vmem_limit_bytes=16 * 1024 * 1024),
        name="triangle",
    )(got)


def tail_kernel(
    product_ref, one_ref, gate_ref, mix_ref, up_ref, down_ref, next_ref,
    out_ref, copied_ref, turned_ref,
):
    step = pl.program_id(0)
    rows, cols, width = one_ref.shape
    _, tokens, _ = product_ref.shape
    inner = down_ref.shape[0]

    @pl.when(step == 0)
    def _():
        turned_ref[...] = normalize(product_ref[...], 0).reshape(width * tokens, cols)
        copied_ref[...] = next_ref[...]

    pair_two = []
    for n in range(rows):
        block = turned_ref[pl.ds(step * rows + n, width, stride=tokens), :].astype(bf16)
        mixed = lax.dot_general(block, mix_ref[...], TN, preferred_element_type=f32)
        pair_two.append((one_ref[n].astype(f32) + gate_ref[n] * mixed).astype(bf16))
    pair_two = jnp.concatenate(pair_two, axis=0)
    normed = normalize(pair_two, 1).astype(bf16)
    first = jnp.dot(normed, up_ref[:, :inner], preferred_element_type=f32)
    second = jnp.dot(normed, up_ref[:, inner:], preferred_element_type=f32)
    hidden = (first * sigmoid(first) * second).astype(bf16)
    update = jnp.dot(hidden, down_ref[...], preferred_element_type=f32)
    out_ref[...] = (pair_two.astype(f32) + update).astype(bf16).reshape(rows, cols, width)


def tail(product, one, gate, mix, up, down, following):
    tokens, cols, width = one.shape
    rows = 4
    pairs = pl.BlockSpec((rows, cols, width), lambda n: (n, 0, 0))
    return pl.pallas_call(
        tail_kernel,
        grid=(tokens // rows,),
        in_specs=[
            whole(product.shape), pairs, pairs, whole(mix.shape), whole(up.shape),
            whole(down.shape), whole(following.shape),
        ],
        out_specs=[pairs, whole(following.shape)],
        out_shape=[
            jax.ShapeDtypeStruct(one.shape, bf16),
            jax.ShapeDtypeStruct(following.shape, bf16),
        ],
        scratch_shapes=[pltpu.VMEM((width * tokens, cols), f32)],
        compiler_params=pltpu.CompilerParams(vmem_limit_bytes=24 * 1024 * 1024),
        name="tail",
    )(product, one, gate, mix, up, down, following)


def swap(value, axis, bit):
    size = lax.axis_size(axis)
    return lax.ppermute(value, axis, [(n, n ^ bit) for n in range(size)])


def flipped(part, col, n_part):
    return jnp.where((part - col) % n_part * 2 == n_part, 1, 0)


def along_rows(own):
    n_part, n_near = lax.axis_size("part"), lax.axis_size("near")
    pairs = []
    for a in range(n_part):
        for n in range(n_near):
            for x in range(n_part):
                b = (x + n // 2 * (n_part // 2) - a) % n_part
                to = n ^ 1 if (b - a) % n_part * 2 == n_part else n
                pairs.append(((a * n_near + n) * n_part + x, (b * n_near + to) * n_part + x))
    return lax.ppermute(own, ("part", "near", "col"), pairs)


def along_columns(value):
    n_part, n_near = lax.axis_size("part"), lax.axis_size("near")
    pairs = []
    for a in range(n_part):
        for n in range(n_near):
            for x in range(n_part):
                to = (x + n // 2 * (n_part // 2) - a) % n_part
                pairs.append(((a * n_near + n) * n_part + x, (a * n_near + n) * n_part + to))
    return lax.ppermute(value, ("part", "near", "col"), pairs)


def gathered_pieces(turned):
    near, core = lax.axis_index("near"), lax.axis_index("core")
    n_part, n_near = lax.axis_size("part"), lax.axis_size("near")
    parts, codes = along_columns(turned)[None], [0]
    bit = n_near // 2
    while bit:
        parts = jnp.concatenate([parts, swap(parts, "near", bit)], axis=0)
        codes = codes + [code ^ bit for code in codes]
        bit //= 2
    other = swap(parts, "core", 1)
    flip = flipped(lax.axis_index("part"), lax.axis_index("col"), n_part)
    place = ((near ^ flip) * 2 + core).astype(jnp.int32)
    codes = [code * 2 for code in codes] + [code * 2 + 1 for code in codes]
    return parts, other, place, codes


def scattered_sum(value, axis):
    size, at = lax.axis_size(axis), lax.axis_index(axis)
    total = lax.dynamic_index_in_dim(value, at, 0, keepdims=False).astype(f32)
    for k in range(1, size):
        piece = lax.dynamic_index_in_dim(value, (at + k) % size, 0, keepdims=False)
        piece = lax.ppermute(piece, axis, [(n, (n + k) % size) for n in range(size)])
        total = total + piece.astype(f32)
    return total


def on_device(
    pair_grid,
    alignment_pool,
    sample_index,
    token_mask,
    outer_proj,
    outer_mix,
    pair_logit,
    average_proj,
    average_mix,
    triangle_proj,
    triangle_mix,
    transition_up,
    transition_down,
):
    n_row = lax.axis_size(ROW)
    n_col = lax.axis_size("col")
    tok_row = pair_grid.shape[0]
    tok_col = pair_grid.shape[1]
    pair_width = pair_grid.shape[2]
    samples = sample_index.shape[0]
    align_width = alignment_pool.shape[2]
    head_count = pair_logit.shape[1]
    head_total = average_proj.shape[1] // 2
    head_dim = head_total // head_count
    quarter = samples // n_col
    sample_start = lax.axis_index("col") * quarter

    norm_t, norm_flat = drawn_alignments(alignment_pool, sample_index)
    turned = along_rows(norm_flat)

    mixed, spread = mixed_rows(norm_t, outer_proj, outer_mix, 16, 4)
    turned, mixed, spread = lax.optimization_barrier((turned, mixed, spread))
    parts, other, place, codes = gathered_pieces(turned)
    row_start = lax.axis_index(ROW) * tok_row
    scalars = [
        value.astype(jnp.int32).reshape(1) for value in (place, row_start, lax.axis_index("col"))
    ]
    pair_one, pair_norm, weights, factors = pair_part(
        scalars + [token_mask], codes, parts, other, spread, mixed, pair_grid, triangle_proj,
        pair_logit.T, token_mask.reshape(n_col, tok_col),
    )

    factors, parts, other, pool, index = lax.optimization_barrier(
        (factors, parts, other, alignment_pool, sample_index)
    )
    received = lax.all_to_all(factors, ROW_COL, split_axis=0, concat_axis=0, tiled=True)

    value_weight = average_proj[:, :head_total].reshape(align_width, head_count, head_dim)
    gate_weight = average_proj[:, head_total:]
    partial_total = jnp.sum(weights, axis=2)
    low_weights = weights.astype(bf16).reshape(tok_row * head_count, tok_col)
    half = tok_col // 2
    drawn = 0.0
    for n, pieces in enumerate((parts, other)):
        row = lax.broadcasted_iota(jnp.int32, (tok_col, half), 0)
        lane = lax.broadcasted_iota(jnp.int32, (tok_col, half), 1)
        code = jnp.repeat(jnp.array(codes[n * len(codes) // 2 :][: half // tok_row]), tok_row)
        source = (place ^ code[None, :]) * tok_row + lane % tok_row
        pick = jnp.where(row == source, 1.0, 0.0).astype(bf16)
        sorted_weights = jnp.dot(low_weights, pick, preferred_element_type=f32).astype(bf16)
        drawn = drawn + jnp.dot(
            sorted_weights, pieces.reshape(half, samples * align_width),
            preferred_element_type=f32,
        )
    drawn = drawn.astype(bf16).reshape(tok_row, head_count, samples, align_width)
    partial_sum = jnp.einsum(
        "ihsm,mhc->sihc", drawn, value_weight, preferred_element_type=f32
    ).astype(bf16).reshape(n_col, quarter, tok_row, head_total)
    high = partial_total.astype(bf16)
    low = (partial_total - high.astype(f32)).astype(bf16)
    total_row = jnp.concatenate([high, low], axis=1)
    total_row = jnp.pad(total_row, ((0, 0), (0, head_total - 2 * head_count)))
    total_row = jnp.broadcast_to(total_row, (n_col, 1, tok_row, head_total))
    sums = jnp.concatenate([partial_sum, total_row], axis=1)
    sums = scattered_sum(sums, "col")
    received, sums = lax.optimization_barrier((received, sums))
    totals = sums[quarter, :, :head_count] + sums[quarter, :, head_count : 2 * head_count]
    weighted = sums[:quarter]
    own_index = lax.dynamic_slice_in_dim(index, sample_start, quarter, 0)
    own_align = jnp.take(pool, own_index, axis=0, mode="clip")
    own_norm = normalize(own_align, 2).astype(bf16)
    gate_values = jax.nn.sigmoid(
        jnp.einsum("sim,mk->sik", own_norm, gate_weight, preferred_element_type=f32)
    )
    share = jnp.repeat(1.0 / totals, head_dim, axis=1)
    averaged = (gate_values * weighted * share).astype(bf16)
    align_update = jnp.einsum("sik,km->sim", averaged, average_mix, preferred_element_type=f32)
    own_next = (own_align.astype(f32) + align_update).astype(bf16)
    alignment_next = lax.all_gather(own_next, "col", axis=0, tiled=True)

    result = triangle(received.reshape(n_row, n_col, 2, tok_row, tok_col))
    product = lax.all_to_all(
        result.reshape(n_row * n_col, tok_row, tok_col), ROW_COL,
        split_axis=0, concat_axis=0, tiled=True,
    )
    flat_norm = pair_norm.reshape(tok_row * tok_col, pair_width)
    gate_out = jax.nn.sigmoid(
        jnp.dot(flat_norm, triangle_proj[:, 4 * pair_width :], preferred_element_type=f32)
    ).reshape(pair_grid.shape)
    return tuple(
        tail(
            product, pair_one, gate_out, triangle_mix, transition_up, transition_down,
            alignment_next,
        )
    )


def solution(mesh):
    n_groups, n_row, n_col = mesh.shape["groups"], mesh.shape["row"], mesh.shape["col"]
    split = Mesh(
        mesh.devices.reshape(n_groups, n_col, n_row // n_col // 2, 2, n_col),
        ("groups", "part", "near", "core", "col"),
    )
    placed = (
        P(GROUPS_ROW, "col", None),
        P("groups", ROW, None),
        P("groups"),
        P("groups"),
    ) + (P(),) * 9
    return jax.shard_map(
        on_device,
        mesh=split,
        in_specs=placed,
        out_specs=(P(GROUPS_ROW, "col", None), P("groups", ROW, None)),
        check_vma=False,
    )
```

```python
import functools

import jax
import jax.numpy as jnp
from jax import lax
from jax.experimental import pallas as pl
from jax.experimental.pallas import tpu as pltpu
from jax.sharding import Mesh
from jax.sharding import PartitionSpec as P

ROW = ("part", "near", "core")
ROW_COL = ("part", "near", "core", "col")
GROUPS_ROW = ("groups", "part", "near", "core")

epsilon = 1e-05
f32 = jnp.float32
bf16 = jnp.bfloat16
NT = (((1,), (1,)), ((), ()))
TN = (((0,), (0,)), ((), ()))


def normalize(values, channel_dim):
    values = values.astype(f32)
    centred = values - jnp.mean(values, axis=channel_dim, keepdims=True)
    spread = jnp.mean(centred * centred, axis=channel_dim, keepdims=True)
    return centred * lax.rsqrt(spread + epsilon)


def sigmoid(x):
    return 1.0 / (1.0 + jnp.exp(-x))


def whole(shape):
    return pl.BlockSpec(shape, lambda *_: (0,) * len(shape))


def draw_kernel(index_ref, pool_ref, turn_ref, flat_ref, normed_ref):
    tokens, samples, width = turn_ref.shape
    stored = pool_ref.shape[2]
    at = lax.broadcasted_iota(jnp.int32, (stored, samples), 0)
    pick = jnp.where(at == index_ref[...], 1.0, 0.0).astype(f32).T.astype(bf16)
    for t in range(tokens):
        drawn = lax.dot_general(pick, pool_ref[t], NT, preferred_element_type=f32)
        normed = normalize(drawn, 1)
        turn_ref[t] = normed.astype(bf16)
        normed_ref[t * samples : (t + 1) * samples, :] = normed
    for s in range(0, samples, 2):
        both = jnp.concatenate(
            [normed_ref[pl.ds(s + n, tokens, stride=samples), :] for n in range(2)], axis=1
        )
        flat_ref[:, s * width : (s + 2) * width] = both.astype(bf16)


def drawn_alignments(pool, index):
    _, tokens, width = pool.shape
    samples = index.shape[0]
    vmem = pl.BlockSpec(memory_space=pltpu.VMEM)
    return pl.pallas_call(
        draw_kernel,
        in_specs=[vmem] * 2,
        out_specs=[vmem] * 2,
        out_shape=[
            jax.ShapeDtypeStruct((tokens, samples, width), bf16),
            jax.ShapeDtypeStruct((tokens, samples * width), bf16),
        ],
        scratch_shapes=[pltpu.VMEM((tokens * samples, width), f32)],
        name="draw",
    )(index.reshape(1, samples), pool.transpose(1, 2, 0))


def ready_kernel(norm_ref, proj_ref, mix_ref, row_ref, mix_t_ref, spread_ref, wide_ref):
    tokens, samples, align = norm_ref.shape
    inner = row_ref.shape[0] // tokens
    depth = mix_ref.shape[0] // inner
    group = spread_ref.shape[0] // depth
    proj_t = proj_ref[...].astype(f32).T
    row_t = proj_t[:inner].astype(bf16)
    for i in range(tokens):
        rows = lax.dot_general(row_t, norm_ref[i], NT, preferred_element_type=f32)
        row_ref[i * inner : (i + 1) * inner, :] = rows.astype(bf16)
    wide_ref[...] = mix_ref[...].astype(f32)
    picked = [wide_ref[pl.ds(d, inner, stride=depth), :] for d in range(depth)]
    mix_t_ref[...] = jnp.concatenate(picked, axis=0).T.astype(bf16)
    turned = proj_t[inner:]
    turned = jnp.concatenate([turned, turned], axis=1)
    turned = jnp.broadcast_to(turned[:, None, :], (depth, group, 2 * align))
    turned = turned.reshape(depth * group, 2 * align)
    row = lax.broadcasted_iota(jnp.int32, turned.shape, 0) % group
    lane = lax.broadcasted_iota(jnp.int32, turned.shape, 1) // align
    for s in range(0, group, 2):
        chunk = jnp.where(row == lane + s, turned, 0.0)
        spread_ref[:, s * align : (s + 2) * align] = chunk.astype(bf16)


def made_ready(norm_t, proj, mix, group):
    tokens, samples, align = norm_t.shape
    depth = proj.shape[1] // 2
    inner = mix.shape[0] // depth
    vmem = pl.BlockSpec(memory_space=pltpu.VMEM)
    return pl.pallas_call(
        ready_kernel,
        in_specs=[vmem] * 3,
        out_specs=[vmem] * 3,
        out_shape=[
            jax.ShapeDtypeStruct((tokens * inner, samples), bf16),
            jax.ShapeDtypeStruct((mix.shape[1], mix.shape[0]), bf16),
            jax.ShapeDtypeStruct((depth * group, group * align), bf16),
        ],
        scratch_shapes=[pltpu.VMEM(mix.shape, f32)],
        cost_estimate=pl.CostEstimate(
            flops=1 << 33, bytes_accessed=1 << 22, transcendentals=0
        ),
        compiler_params=pltpu.CompilerParams(vmem_limit_bytes=16 * 1024 * 1024),
        name="made_ready",
    )(norm_t, proj, mix)


def pair_kernel(
    place_ref, first_ref, side_ref, token_ref,
    own_ref, other_ref, spread_ref, row_ref, mix_ref, pair_ref, proj_ref, logit_ref, mask_ref,
    one_ref, pnorm_ref, weight_ref, factor_ref,
    sorted_ref, col_ref, outer_ref, proj_t_ref, left_ref, right_ref, made_ref, out_sem,
    *, codes,
):
    step = pl.program_id(0)
    rows, cols, width = pair_ref.shape
    tokens = made_ref.shape[2]
    got, chunk = spread_ref.shape
    kept = own_ref.shape[0]
    samples = row_ref.shape[1]
    inner = row_ref.shape[0] // tokens
    depth = mix_ref.shape[1] // inner
    group = got // depth

    @pl.when(step == 0)
    def _():
        proj_t_ref[...] = proj_ref[:, : 4 * width].astype(f32).T.astype(bf16)
        for n, code in enumerate(codes):
            at = pl.multiple_of((place_ref[0] ^ code) * tokens, tokens)
            piece = own_ref[n] if n < kept else other_ref[n - kept]
            sorted_ref[pl.ds(at, tokens), :] = piece
        for g in range(sorted_ref.shape[1] // chunk):
            part = lax.dot_general(
                sorted_ref[:, g * chunk : (g + 1) * chunk], spread_ref[...], NT,
                preferred_element_type=f32,
            )
            part = part.T.astype(bf16)
            for d in range(depth):
                col_ref[g * group : (g + 1) * group, d * cols : (d + 1) * cols] = part[
                    d * group : (d + 1) * group
                ]

    block = row_ref[pl.ds(pl.multiple_of(step * rows * inner, rows * inner), rows * inner), :]
    for d in range(0, depth, 2):
        outer = jnp.dot(
            block, col_ref[:, d * cols : (d + 2) * cols], preferred_element_type=f32
        ) * (1.0 / samples)
        outer = outer.astype(bf16)
        for more in range(2):
            for i in range(rows):
                at = (d + more) * inner
                outer_ref[i // 2, at : at + inner, (i % 2) * cols : (i % 2 + 1) * cols] = outer[
                    i * inner : (i + 1) * inner, more * cols : (more + 1) * cols
                ]
    updates = []
    for n in range(rows // 2):
        both = jnp.dot(mix_ref[...], outer_ref[n], preferred_element_type=f32)
        updates += [both[:, :cols].T, both[:, cols:].T]
    normed = []
    for n in range(rows):
        one = (pair_ref[n].astype(f32) + updates[n]).astype(bf16)
        one_ref[n] = one
        now = normalize(one, 1).astype(bf16)
        pnorm_ref[n] = now
        normed.append(now)
    normed = jnp.concatenate(normed, axis=0)
    projected = lax.dot_general(proj_t_ref[...], normed, NT, preferred_element_type=f32)
    scores = jnp.exp(lax.dot_general(logit_ref[...], normed, NT, preferred_element_type=f32))
    left = sigmoid(projected[:width]) * projected[width : 2 * width]
    right = sigmoid(projected[2 * width : 3 * width]) * projected[3 * width :]
    column_mask = mask_ref[pl.ds(side_ref[0], 1), :].astype(f32)
    for n in range(rows):
        weight_ref[n] = scores[:, n * cols : (n + 1) * cols]
        mask = column_mask * token_ref[first_ref[0] + step * rows + n].astype(f32)
        lanes = slice(n * cols, (n + 1) * cols)
        at = pl.ds(step * rows + n, width, stride=tokens)
        left_ref[at, :] = left[:, lanes] * mask
        right_ref[at, :] = right[:, lanes] * mask

    @pl.when(step == pl.num_programs(0) - 1)
    def _():
        sends = out_sem.shape[0]
        share = width // sends
        copies = []
        for n in range(sends):
            own = slice(n * share, (n + 1) * share)
            for side, ref in enumerate((left_ref, right_ref)):
                block = ref[n * share * tokens : (n + 1) * share * tokens, :]
                made_ref[own, side] = block.reshape(share, tokens, cols).astype(bf16)
            copy = pltpu.make_async_copy(
                made_ref.at[pl.ds(n * share, share)], factor_ref.at[pl.ds(n * share, share)],
                out_sem.at[n],
            )
            copy.start()
            copies.append(copy)
        for copy in copies:
            copy.wait()


def pair_part(scalars, codes, own, other, spread, row, mix, pair_grid, proj, logit_t, mask):
    tokens, cols, width = pair_grid.shape
    heads = logit_t.shape[0]
    rows = 4
    steps = tokens // rows
    samples = row.shape[1]
    pairs = pl.BlockSpec((rows, cols, width), lambda n, *_: (n, 0, 0))
    anywhere = pl.BlockSpec(memory_space=pltpu.HBM)
    return pl.pallas_call(
        functools.partial(pair_kernel, codes=codes),
        grid_spec=pltpu.PrefetchScalarGridSpec(
            num_scalar_prefetch=4,
            grid=(steps,),
            in_specs=[
                whole(own.shape),
                whole(other.shape),
                whole(spread.shape),
                whole(row.shape),
                whole(mix.shape),
                pairs,
                whole(proj.shape),
                whole(logit_t.shape),
                whole(mask.shape),
            ],
            out_specs=[
                pairs,
                pairs,
                pl.BlockSpec((rows, heads, cols), lambda n, *_: (n, 0, 0)),
                anywhere,
            ],
            scratch_shapes=[
                pltpu.VMEM((cols, own.shape[2]), bf16),
                pltpu.VMEM((samples, mix.shape[1] * tokens // row.shape[0] * cols), bf16),
                pltpu.VMEM((rows // 2, mix.shape[1], 2 * cols), bf16),
                pltpu.VMEM((4 * width, width), bf16),
                pltpu.VMEM((width * tokens, cols), f32),
                pltpu.VMEM((width * tokens, cols), f32),
                pltpu.VMEM((width, 2, tokens, cols), bf16),
                pltpu.SemaphoreType.DMA((8,)),
            ],
        ),
        out_shape=[
            jax.ShapeDtypeStruct(pair_grid.shape, bf16),
            jax.ShapeDtypeStruct(pair_grid.shape, bf16),
            jax.ShapeDtypeStruct((tokens, heads, cols), f32),
            jax.ShapeDtypeStruct((width, 2, tokens, cols), bf16),
        ],
        compiler_params=pltpu.CompilerParams(vmem_limit_bytes=32 * 1024 * 1024),
        name="pair_part",
    )(*scalars, own, other, spread, row, mix, pair_grid, proj, logit_t, mask)


def triangle_kernel(got_ref, out_ref):
    n_row, n_col, _, tokens, cols = got_ref.shape
    sides = []
    for side in range(2):
        sides.append(
            jnp.concatenate(
                [got_ref[:, x, side].reshape(n_row * tokens, cols) for x in range(n_col)], axis=1
            )
        )
    product = lax.dot_general(sides[0], sides[1], NT, preferred_element_type=f32).astype(bf16)
    for x in range(n_col):
        out_ref[:, x] = product[:, x * cols : (x + 1) * cols].reshape(n_row, tokens, cols)


def triangle(got):
    n_row, n_col, _, tokens, cols = got.shape
    return pl.pallas_call(
        triangle_kernel,
        out_shape=jax.ShapeDtypeStruct((n_row, n_col, tokens, cols), bf16),
        in_specs=[pl.BlockSpec(memory_space=pltpu.VMEM)],
        out_specs=pl.BlockSpec(memory_space=pltpu.VMEM),
        compiler_params=pltpu.CompilerParams(vmem_limit_bytes=16 * 1024 * 1024),
        name="triangle",
    )(got)


def tail_kernel(
    product_ref, one_ref, gate_ref, mix_ref, up_ref, down_ref, next_ref,
    out_ref, copied_ref, turned_ref,
):
    step = pl.program_id(0)
    rows, cols, width = one_ref.shape
    _, tokens, _ = product_ref.shape
    inner = down_ref.shape[0]

    @pl.when(step == 0)
    def _():
        turned_ref[...] = normalize(product_ref[...], 0).reshape(width * tokens, cols)
        copied_ref[...] = next_ref[...]

    pair_two = []
    for n in range(rows):
        block = turned_ref[pl.ds(step * rows + n, width, stride=tokens), :].astype(bf16)
        mixed = lax.dot_general(block, mix_ref[...], TN, preferred_element_type=f32)
        pair_two.append((one_ref[n].astype(f32) + gate_ref[n] * mixed).astype(bf16))
    pair_two = jnp.concatenate(pair_two, axis=0)
    normed = normalize(pair_two, 1).astype(bf16)
    first = jnp.dot(normed, up_ref[:, :inner], preferred_element_type=f32)
    second = jnp.dot(normed, up_ref[:, inner:], preferred_element_type=f32)
    hidden = (first * sigmoid(first) * second).astype(bf16)
    update = jnp.dot(hidden, down_ref[...], preferred_element_type=f32)
    out_ref[...] = (pair_two.astype(f32) + update).astype(bf16).reshape(rows, cols, width)


def tail(product, one, gate, mix, up, down, following):
    tokens, cols, width = one.shape
    rows = 4
    pairs = pl.BlockSpec((rows, cols, width), lambda n: (n, 0, 0))
    return pl.pallas_call(
        tail_kernel,
        grid=(tokens // rows,),
        in_specs=[
            whole(product.shape), pairs, pairs, whole(mix.shape), whole(up.shape),
            whole(down.shape), whole(following.shape),
        ],
        out_specs=[pairs, whole(following.shape)],
        out_shape=[
            jax.ShapeDtypeStruct(one.shape, bf16),
            jax.ShapeDtypeStruct(following.shape, bf16),
        ],
        scratch_shapes=[pltpu.VMEM((width * tokens, cols), f32)],
        compiler_params=pltpu.CompilerParams(vmem_limit_bytes=24 * 1024 * 1024),
        name="tail",
    )(product, one, gate, mix, up, down, following)


def swap(value, axis, bit):
    size = lax.axis_size(axis)
    return lax.ppermute(value, axis, [(n, n ^ bit) for n in range(size)])


def flipped(part, col, n_part):
    return jnp.where((part - col) % n_part * 2 == n_part, 1, 0)


def along_rows(own):
    n_part, n_near = lax.axis_size("part"), lax.axis_size("near")
    pairs = []
    for a in range(n_part):
        for n in range(n_near):
            for x in range(n_part):
                b = (x + n // 2 * (n_part // 2) - a) % n_part
                to = n ^ 1 if (b - a) % n_part * 2 == n_part else n
                pairs.append(((a * n_near + n) * n_part + x, (b * n_near + to) * n_part + x))
    return lax.ppermute(own, ("part", "near", "col"), pairs)


def along_columns(value):
    n_part, n_near = lax.axis_size("part"), lax.axis_size("near")
    pairs = []
    for a in range(n_part):
        for n in range(n_near):
            for x in range(n_part):
                to = (x + n // 2 * (n_part // 2) - a) % n_part
                pairs.append(((a * n_near + n) * n_part + x, (a * n_near + n) * n_part + to))
    return lax.ppermute(value, ("part", "near", "col"), pairs)


def join_kernel(first_ref, second_ref, out_ref):
    count = first_ref.shape[0]
    out_ref[:count] = first_ref[...]
    out_ref[count:] = second_ref[...]


def joined(first, second):
    vmem = pl.BlockSpec(memory_space=pltpu.VMEM)
    return pl.pallas_call(
        join_kernel,
        in_specs=[vmem] * 2,
        out_specs=vmem,
        out_shape=jax.ShapeDtypeStruct((first.shape[0] * 2,) + first.shape[1:], bf16),
        compiler_params=pltpu.CompilerParams(vmem_limit_bytes=8 * 1024 * 1024),
        name="joined",
    )(first, second)


def gathered_pieces(turned):
    near, core = lax.axis_index("near"), lax.axis_index("core")
    n_part, n_near = lax.axis_size("part"), lax.axis_size("near")
    parts, codes = along_columns(turned)[None], [0]
    bit = n_near // 2
    while bit:
        parts = joined(parts, swap(parts, "near", bit))
        codes = codes + [code ^ bit for code in codes]
        bit //= 2
    other = swap(parts, "core", 1)
    flip = flipped(lax.axis_index("part"), lax.axis_index("col"), n_part)
    place = ((near ^ flip) * 2 + core).astype(jnp.int32)
    codes = [code * 2 for code in codes] + [code * 2 + 1 for code in codes]
    return parts, other, place, codes


def scattered_sum(value, axis):
    size, at = lax.axis_size(axis), lax.axis_index(axis)
    total = lax.dynamic_index_in_dim(value, at, 0, keepdims=False).astype(f32)
    for k in range(1, size):
        piece = lax.dynamic_index_in_dim(value, (at + k) % size, 0, keepdims=False)
        piece = lax.ppermute(piece, axis, [(n, (n + k) % size) for n in range(size)])
        total = total + piece.astype(f32)
    return total


def on_device(
    pair_grid,
    alignment_pool,
    sample_index,
    token_mask,
    outer_proj,
    outer_mix,
    pair_logit,
    average_proj,
    average_mix,
    triangle_proj,
    triangle_mix,
    transition_up,
    transition_down,
):
    n_row = lax.axis_size(ROW)
    n_col = lax.axis_size("col")
    tok_row = pair_grid.shape[0]
    tok_col = pair_grid.shape[1]
    pair_width = pair_grid.shape[2]
    samples = sample_index.shape[0]
    align_width = alignment_pool.shape[2]
    head_count = pair_logit.shape[1]
    head_total = average_proj.shape[1] // 2
    head_dim = head_total // head_count
    quarter = samples // n_col
    sample_start = lax.axis_index("col") * quarter

    norm_t, norm_flat = drawn_alignments(alignment_pool, sample_index)
    turned = along_rows(norm_flat)

    row, mix_t, spread = made_ready(norm_t, outer_proj, outer_mix, 16)
    turned, row, mix_t, spread = lax.optimization_barrier((turned, row, mix_t, spread))
    parts, other, place, codes = gathered_pieces(turned)
    row_start = lax.axis_index(ROW) * tok_row
    scalars = [
        value.astype(jnp.int32).reshape(1) for value in (place, row_start, lax.axis_index("col"))
    ]
    pair_one, pair_norm, weights, factors = pair_part(
        scalars + [token_mask], codes, parts, other, spread, row, mix_t, pair_grid, triangle_proj,
        pair_logit.T, token_mask.reshape(n_col, tok_col),
    )

    factors, parts, other, pool, index = lax.optimization_barrier(
        (factors, parts, other, alignment_pool, sample_index)
    )
    received = lax.all_to_all(factors, ROW_COL, split_axis=0, concat_axis=0, tiled=True)

    value_weight = average_proj[:, :head_total].reshape(align_width, head_count, head_dim)
    gate_weight = average_proj[:, head_total:]
    partial_total = jnp.sum(weights, axis=2)
    low_weights = weights.astype(bf16).reshape(tok_row * head_count, tok_col)
    half = tok_col // 2
    drawn = 0.0
    for n, pieces in enumerate((parts, other)):
        row = lax.broadcasted_iota(jnp.int32, (tok_col, half), 0)
        lane = lax.broadcasted_iota(jnp.int32, (tok_col, half), 1)
        code = jnp.repeat(jnp.array(codes[n * len(codes) // 2 :][: half // tok_row]), tok_row)
        source = (place ^ code[None, :]) * tok_row + lane % tok_row
        pick = jnp.where(row == source, 1.0, 0.0).astype(bf16)
        sorted_weights = jnp.dot(low_weights, pick, preferred_element_type=f32).astype(bf16)
        drawn = drawn + jnp.dot(
            sorted_weights, pieces.reshape(half, samples * align_width),
            preferred_element_type=f32,
        )
    drawn = drawn.astype(bf16).reshape(tok_row, head_count, samples, align_width)
    partial_sum = jnp.einsum(
        "ihsm,mhc->sihc", drawn, value_weight, preferred_element_type=f32
    ).astype(bf16).reshape(n_col, quarter, tok_row, head_total)
    high = partial_total.astype(bf16)
    low = (partial_total - high.astype(f32)).astype(bf16)
    total_row = jnp.concatenate([high, low], axis=1)
    total_row = jnp.pad(total_row, ((0, 0), (0, head_total - 2 * head_count)))
    total_row = jnp.broadcast_to(total_row, (n_col, 1, tok_row, head_total))
    sums = jnp.concatenate([partial_sum, total_row], axis=1)
    sums = scattered_sum(sums, "col")
    received, sums = lax.optimization_barrier((received, sums))
    totals = sums[quarter, :, :head_count] + sums[quarter, :, head_count : 2 * head_count]
    weighted = sums[:quarter]
    own_index = lax.dynamic_slice_in_dim(index, sample_start, quarter, 0)
    own_align = jnp.take(pool, own_index, axis=0, mode="clip")
    own_norm = normalize(own_align, 2).astype(bf16)
    gate_values = jax.nn.sigmoid(
        jnp.einsum("sim,mk->sik", own_norm, gate_weight, preferred_element_type=f32)
    )
    share = jnp.repeat(1.0 / totals, head_dim, axis=1)
    averaged = (gate_values * weighted * share).astype(bf16)
    align_update = jnp.einsum("sik,km->sim", averaged, average_mix, preferred_element_type=f32)
    own_next = (own_align.astype(f32) + align_update).astype(bf16)
    alignment_next = lax.all_gather(own_next, "col", axis=0, tiled=True)

    result = triangle(received.reshape(n_row, n_col, 2, tok_row, tok_col))
    product = lax.all_to_all(
        result.reshape(n_row * n_col, tok_row, tok_col), ROW_COL,
        split_axis=0, concat_axis=0, tiled=True,
    )
    flat_norm = pair_norm.reshape(tok_row * tok_col, pair_width)
    gate_out = jax.nn.sigmoid(
        jnp.dot(flat_norm, triangle_proj[:, 4 * pair_width :], preferred_element_type=f32)
    ).reshape(pair_grid.shape)
    return tuple(
        tail(
            product, pair_one, gate_out, triangle_mix, transition_up, transition_down,
            alignment_next,
        )
    )


def solution(mesh):
    n_groups, n_row, n_col = mesh.shape["groups"], mesh.shape["row"], mesh.shape["col"]
    split = Mesh(
        mesh.devices.reshape(n_groups, n_col, n_row // n_col // 2, 2, n_col),
        ("groups", "part", "near", "core", "col"),
    )
    placed = (
        P(GROUPS_ROW, "col", None),
        P("groups", ROW, None),
        P("groups"),
        P("groups"),
    ) + (P(),) * 9
    return jax.shard_map(
        on_device,
        mesh=split,
        in_specs=placed,
        out_specs=(P(GROUPS_ROW, "col", None), P("groups", ROW, None)),
        check_vma=False,
    )
```

```python
import functools

import jax
import jax.numpy as jnp
from jax import lax
from jax.experimental import pallas as pl
from jax.experimental.pallas import tpu as pltpu
from jax.sharding import Mesh
from jax.sharding import PartitionSpec as P

ROW = ("part", "near", "core")
ROW_COL = ("part", "near", "core", "col")
GROUPS_ROW = ("groups", "part", "near", "core")

epsilon = 1e-05
f32 = jnp.float32
bf16 = jnp.bfloat16
NT = (((1,), (1,)), ((), ()))
TN = (((0,), (0,)), ((), ()))


def normalize(values, channel_dim):
    values = values.astype(f32)
    centred = values - jnp.mean(values, axis=channel_dim, keepdims=True)
    spread = jnp.mean(centred * centred, axis=channel_dim, keepdims=True)
    return centred * lax.rsqrt(spread + epsilon)


def sigmoid(x):
    return 1.0 / (1.0 + jnp.exp(-x))


def whole(shape):
    return pl.BlockSpec(shape, lambda *_: (0,) * len(shape))


def draw_kernel(index_ref, pool_ref, turn_ref, flat_ref, normed_ref):
    tokens, samples, width = turn_ref.shape
    stored = pool_ref.shape[2]
    at = lax.broadcasted_iota(jnp.int32, (stored, samples), 0)
    pick = jnp.where(at == index_ref[...], 1.0, 0.0).astype(f32).T.astype(bf16)
    for t in range(tokens):
        drawn = lax.dot_general(pick, pool_ref[t], NT, preferred_element_type=f32)
        normed = normalize(drawn, 1)
        turn_ref[t] = normed.astype(bf16)
        normed_ref[t * samples : (t + 1) * samples, :] = normed
    for s in range(0, samples, 2):
        both = jnp.concatenate(
            [normed_ref[pl.ds(s + n, tokens, stride=samples), :] for n in range(2)], axis=1
        )
        flat_ref[:, s * width : (s + 2) * width] = both.astype(bf16)


def drawn_alignments(pool, index):
    _, tokens, width = pool.shape
    samples = index.shape[0]
    vmem = pl.BlockSpec(memory_space=pltpu.VMEM)
    return pl.pallas_call(
        draw_kernel,
        in_specs=[vmem] * 2,
        out_specs=[vmem] * 2,
        out_shape=[
            jax.ShapeDtypeStruct((tokens, samples, width), bf16),
            jax.ShapeDtypeStruct((tokens, samples * width), bf16),
        ],
        scratch_shapes=[pltpu.VMEM((tokens * samples, width), f32)],
        name="draw",
    )(index.reshape(1, samples), pool.transpose(1, 2, 0))


def ready_kernel(norm_ref, proj_ref, mix_ref, gates_ref, mix_t_ref, pack_ref, wide_ref):
    tokens, samples, align = norm_ref.shape
    width = mix_ref.shape[1]
    inner = pack_ref.shape[0] // tokens
    depth = mix_ref.shape[0] // inner
    group = pack_ref.shape[0] // depth
    chunk = group * align
    proj_t = proj_ref[...].astype(f32).T
    row_t = proj_t[:inner].astype(bf16)
    for i in range(tokens):
        rows = lax.dot_general(row_t, norm_ref[i], NT, preferred_element_type=f32)
        pack_ref[i * inner : (i + 1) * inner, chunk : chunk + samples] = rows.astype(bf16)
    pack_ref[:, chunk + width :] = gates_ref[:, : 4 * width].astype(f32).T.astype(bf16)
    wide_ref[...] = mix_ref[...].astype(f32)
    picked = [wide_ref[pl.ds(d, inner, stride=depth), :] for d in range(depth)]
    mix_t_ref[...] = jnp.concatenate(picked, axis=0).T.astype(bf16)
    turned = proj_t[inner:]
    turned = jnp.concatenate([turned, turned], axis=1)
    turned = jnp.broadcast_to(turned[:, None, :], (depth, group, 2 * align))
    turned = turned.reshape(depth * group, 2 * align)
    row = lax.broadcasted_iota(jnp.int32, turned.shape, 0) % group
    lane = lax.broadcasted_iota(jnp.int32, turned.shape, 1) // align
    for s in range(0, group, 2):
        kept = jnp.where(row == lane + s, turned, 0.0)
        pack_ref[:, s * align : (s + 2) * align] = kept.astype(bf16)


def made_ready(norm_t, proj, mix, gates, group):
    tokens, samples, align = norm_t.shape
    depth = proj.shape[1] // 2
    inner = mix.shape[0] // depth
    vmem = pl.BlockSpec(memory_space=pltpu.VMEM)
    return pl.pallas_call(
        ready_kernel,
        in_specs=[vmem] * 4,
        out_specs=[vmem] * 2,
        out_shape=[
            jax.ShapeDtypeStruct((mix.shape[1], mix.shape[0]), bf16),
            jax.ShapeDtypeStruct((depth * group, group * align + 2 * mix.shape[1]), bf16),
        ],
        scratch_shapes=[pltpu.VMEM(mix.shape, f32)],
        cost_estimate=pl.CostEstimate(
            flops=1 << 33, bytes_accessed=1 << 22, transcendentals=0
        ),
        compiler_params=pltpu.CompilerParams(vmem_limit_bytes=16 * 1024 * 1024),
        name="made_ready",
    )(norm_t, proj, mix, gates)


def pair_kernel(
    place_ref, first_ref, side_ref, token_ref,
    own_ref, other_ref, pack_ref, mix_ref, pair_ref, logit_ref, mask_ref,
    one_ref, pnorm_ref, weight_ref, factor_ref,
    sorted_ref, col_ref, outer_ref, left_ref, right_ref, made_ref, out_sem,
    *, codes,
):
    step = pl.program_id(0)
    rows, cols, width = pair_ref.shape
    tokens = made_ref.shape[2]
    got, chunk = pack_ref.shape[0], pack_ref.shape[1] - 2 * width
    kept = own_ref.shape[0]
    samples = col_ref.shape[0]
    inner = got // tokens
    depth = mix_ref.shape[1] // inner
    group = got // depth

    @pl.when(step == 0)
    def _():
        for n, code in enumerate(codes):
            at = pl.multiple_of((place_ref[0] ^ code) * tokens, tokens)
            piece = own_ref[n] if n < kept else other_ref[n - kept]
            sorted_ref[pl.ds(at, tokens), :] = piece
        for g in range(sorted_ref.shape[1] // chunk):
            part = lax.dot_general(
                sorted_ref[:, g * chunk : (g + 1) * chunk], pack_ref[:, :chunk], NT,
                preferred_element_type=f32,
            )
            part = part.T.astype(bf16)
            for d in range(depth):
                col_ref[g * group : (g + 1) * group, d * cols : (d + 1) * cols] = part[
                    d * group : (d + 1) * group
                ]

    mine = pl.ds(pl.multiple_of(step * rows * inner, rows * inner), rows * inner)
    block = pack_ref[mine, chunk : chunk + samples]
    for d in range(0, depth, 2):
        outer = jnp.dot(
            block, col_ref[:, d * cols : (d + 2) * cols], preferred_element_type=f32
        ) * (1.0 / samples)
        outer = outer.astype(bf16)
        for more in range(2):
            for i in range(rows):
                at = (d + more) * inner
                outer_ref[i // 2, at : at + inner, (i % 2) * cols : (i % 2 + 1) * cols] = outer[
                    i * inner : (i + 1) * inner, more * cols : (more + 1) * cols
                ]
    updates = []
    for n in range(rows // 2):
        both = jnp.dot(mix_ref[...], outer_ref[n], preferred_element_type=f32)
        updates += [both[:, :cols].T, both[:, cols:].T]
    normed = []
    for n in range(rows):
        one = (pair_ref[n].astype(f32) + updates[n]).astype(bf16)
        one_ref[n] = one
        now = normalize(one, 1).astype(bf16)
        pnorm_ref[n] = now
        normed.append(now)
    normed = jnp.concatenate(normed, axis=0)
    projected = lax.dot_general(
        pack_ref[:, chunk + width :], normed, NT, preferred_element_type=f32
    )
    scores = jnp.exp(lax.dot_general(logit_ref[...], normed, NT, preferred_element_type=f32))
    left = sigmoid(projected[:width]) * projected[width : 2 * width]
    right = sigmoid(projected[2 * width : 3 * width]) * projected[3 * width :]
    column_mask = mask_ref[pl.ds(side_ref[0], 1), :].astype(f32)
    for n in range(rows):
        weight_ref[n] = scores[:, n * cols : (n + 1) * cols]
        mask = column_mask * token_ref[first_ref[0] + step * rows + n].astype(f32)
        lanes = slice(n * cols, (n + 1) * cols)
        at = pl.ds(step * rows + n, width, stride=tokens)
        left_ref[at, :] = left[:, lanes] * mask
        right_ref[at, :] = right[:, lanes] * mask

    @pl.when(step == pl.num_programs(0) - 1)
    def _():
        sends = out_sem.shape[0]
        share = width // sends
        copies = []
        for n in range(sends):
            own = slice(n * share, (n + 1) * share)
            for side, ref in enumerate((left_ref, right_ref)):
                block = ref[n * share * tokens : (n + 1) * share * tokens, :]
                made_ref[own, side] = block.reshape(share, tokens, cols).astype(bf16)
            copy = pltpu.make_async_copy(
                made_ref.at[pl.ds(n * share, share)], factor_ref.at[pl.ds(n * share, share)],
                out_sem.at[n],
            )
            copy.start()
            copies.append(copy)
        for copy in copies:
            copy.wait()


def pair_part(scalars, codes, own, other, pack, mix, samples, pair_grid, logit_t, mask):
    tokens, cols, width = pair_grid.shape
    heads = logit_t.shape[0]
    rows = 4
    steps = tokens // rows
    inner = pack.shape[0] // tokens
    pairs = pl.BlockSpec((rows, cols, width), lambda n, *_: (n, 0, 0))
    anywhere = pl.BlockSpec(memory_space=pltpu.HBM)
    return pl.pallas_call(
        functools.partial(pair_kernel, codes=codes),
        grid_spec=pltpu.PrefetchScalarGridSpec(
            num_scalar_prefetch=4,
            grid=(steps,),
            in_specs=[
                whole(own.shape),
                whole(other.shape),
                whole(pack.shape),
                whole(mix.shape),
                pairs,
                whole(logit_t.shape),
                whole(mask.shape),
            ],
            out_specs=[
                pairs,
                pairs,
                pl.BlockSpec((rows, heads, cols), lambda n, *_: (n, 0, 0)),
                anywhere,
            ],
            scratch_shapes=[
                pltpu.VMEM((cols, own.shape[2]), bf16),
                pltpu.VMEM((samples, mix.shape[1] // inner * cols), bf16),
                pltpu.VMEM((rows // 2, mix.shape[1], 2 * cols), bf16),
                pltpu.VMEM((width * tokens, cols), f32),
                pltpu.VMEM((width * tokens, cols), f32),
                pltpu.VMEM((width, 2, tokens, cols), bf16),
                pltpu.SemaphoreType.DMA((8,)),
            ],
        ),
        out_shape=[
            jax.ShapeDtypeStruct(pair_grid.shape, bf16),
            jax.ShapeDtypeStruct(pair_grid.shape, bf16),
            jax.ShapeDtypeStruct((tokens, heads, cols), f32),
            jax.ShapeDtypeStruct((width, 2, tokens, cols), bf16),
        ],
        compiler_params=pltpu.CompilerParams(vmem_limit_bytes=32 * 1024 * 1024),
        name="pair_part",
    )(*scalars, own, other, pack, mix, pair_grid, logit_t, mask)


def triangle_kernel(got_ref, out_ref):
    n_row, n_col, _, tokens, cols = got_ref.shape
    sides = []
    for side in range(2):
        sides.append(
            jnp.concatenate(
                [got_ref[:, x, side].reshape(n_row * tokens, cols) for x in range(n_col)], axis=1
            )
        )
    product = lax.dot_general(sides[0], sides[1], NT, preferred_element_type=f32).astype(bf16)
    for x in range(n_col):
        out_ref[:, x] = product[:, x * cols : (x + 1) * cols].reshape(n_row, tokens, cols)


def triangle(got):
    n_row, n_col, _, tokens, cols = got.shape
    return pl.pallas_call(
        triangle_kernel,
        out_shape=jax.ShapeDtypeStruct((n_row, n_col, tokens, cols), bf16),
        in_specs=[pl.BlockSpec(memory_space=pltpu.VMEM)],
        out_specs=pl.BlockSpec(memory_space=pltpu.VMEM),
        compiler_params=pltpu.CompilerParams(vmem_limit_bytes=16 * 1024 * 1024),
        name="triangle",
    )(got)


def tail_kernel(
    product_ref, one_ref, gate_ref, mix_ref, up_ref, down_ref, next_ref,
    out_ref, copied_ref, turned_ref,
):
    step = pl.program_id(0)
    rows, cols, width = one_ref.shape
    _, tokens, _ = product_ref.shape
    inner = down_ref.shape[0]

    @pl.when(step == 0)
    def _():
        turned_ref[...] = normalize(product_ref[...], 0).reshape(width * tokens, cols)
        copied_ref[...] = next_ref[...]

    pair_two = []
    for n in range(rows):
        block = turned_ref[pl.ds(step * rows + n, width, stride=tokens), :].astype(bf16)
        mixed = lax.dot_general(block, mix_ref[...], TN, preferred_element_type=f32)
        pair_two.append((one_ref[n].astype(f32) + gate_ref[n] * mixed).astype(bf16))
    pair_two = jnp.concatenate(pair_two, axis=0)
    normed = normalize(pair_two, 1).astype(bf16)
    first = jnp.dot(normed, up_ref[:, :inner], preferred_element_type=f32)
    second = jnp.dot(normed, up_ref[:, inner:], preferred_element_type=f32)
    hidden = (first * sigmoid(first) * second).astype(bf16)
    update = jnp.dot(hidden, down_ref[...], preferred_element_type=f32)
    out_ref[...] = (pair_two.astype(f32) + update).astype(bf16).reshape(rows, cols, width)


def tail(product, one, gate, mix, up, down, following):
    tokens, cols, width = one.shape
    rows = 4
    pairs = pl.BlockSpec((rows, cols, width), lambda n: (n, 0, 0))
    return pl.pallas_call(
        tail_kernel,
        grid=(tokens // rows,),
        in_specs=[
            whole(product.shape), pairs, pairs, whole(mix.shape), whole(up.shape),
            whole(down.shape), whole(following.shape),
        ],
        out_specs=[pairs, whole(following.shape)],
        out_shape=[
            jax.ShapeDtypeStruct(one.shape, bf16),
            jax.ShapeDtypeStruct(following.shape, bf16),
        ],
        scratch_shapes=[pltpu.VMEM((width * tokens, cols), f32)],
        compiler_params=pltpu.CompilerParams(vmem_limit_bytes=24 * 1024 * 1024),
        name="tail",
    )(product, one, gate, mix, up, down, following)


def swap(value, axis, bit):
    size = lax.axis_size(axis)
    return lax.ppermute(value, axis, [(n, n ^ bit) for n in range(size)])


def flipped(part, col, n_part):
    return jnp.where((part - col) % n_part * 2 == n_part, 1, 0)


def along_rows(own):
    n_part, n_near = lax.axis_size("part"), lax.axis_size("near")
    pairs = []
    for a in range(n_part):
        for n in range(n_near):
            for x in range(n_part):
                b = (x + n // 2 * (n_part // 2) - a) % n_part
                to = n ^ 1 if (b - a) % n_part * 2 == n_part else n
                pairs.append(((a * n_near + n) * n_part + x, (b * n_near + to) * n_part + x))
    return lax.ppermute(own, ("part", "near", "col"), pairs)


def along_columns(value):
    n_part, n_near = lax.axis_size("part"), lax.axis_size("near")
    pairs = []
    for a in range(n_part):
        for n in range(n_near):
            for x in range(n_part):
                to = (x + n // 2 * (n_part // 2) - a) % n_part
                pairs.append(((a * n_near + n) * n_part + x, (a * n_near + n) * n_part + to))
    return lax.ppermute(value, ("part", "near", "col"), pairs)


def join_kernel(first_ref, second_ref, out_ref):
    count = first_ref.shape[0]
    out_ref[:count] = first_ref[...]
    out_ref[count:] = second_ref[...]


def joined(first, second):
    vmem = pl.BlockSpec(memory_space=pltpu.VMEM)
    return pl.pallas_call(
        join_kernel,
        in_specs=[vmem] * 2,
        out_specs=vmem,
        out_shape=jax.ShapeDtypeStruct((first.shape[0] * 2,) + first.shape[1:], bf16),
        compiler_params=pltpu.CompilerParams(vmem_limit_bytes=8 * 1024 * 1024),
        name="joined",
    )(first, second)


def gathered_pieces(turned):
    near, core = lax.axis_index("near"), lax.axis_index("core")
    n_part, n_near = lax.axis_size("part"), lax.axis_size("near")
    parts, codes = along_columns(turned)[None], [0]
    bit = n_near // 2
    while bit:
        parts = joined(parts, swap(parts, "near", bit))
        codes = codes + [code ^ bit for code in codes]
        bit //= 2
    other = swap(parts, "core", 1)
    flip = flipped(lax.axis_index("part"), lax.axis_index("col"), n_part)
    place = ((near ^ flip) * 2 + core).astype(jnp.int32)
    codes = [code * 2 for code in codes] + [code * 2 + 1 for code in codes]
    return parts, other, place, codes


def scattered_sum(value, axis):
    size, at = lax.axis_size(axis), lax.axis_index(axis)
    total = lax.dynamic_index_in_dim(value, at, 0, keepdims=False).astype(f32)
    for k in range(1, size):
        piece = lax.dynamic_index_in_dim(value, (at + k) % size, 0, keepdims=False)
        piece = lax.ppermute(piece, axis, [(n, (n + k) % size) for n in range(size)])
        total = total + piece.astype(f32)
    return total


def on_device(
    pair_grid,
    alignment_pool,
    sample_index,
    token_mask,
    outer_proj,
    outer_mix,
    pair_logit,
    average_proj,
    average_mix,
    triangle_proj,
    triangle_mix,
    transition_up,
    transition_down,
):
    n_row = lax.axis_size(ROW)
    n_col = lax.axis_size("col")
    tok_row = pair_grid.shape[0]
    tok_col = pair_grid.shape[1]
    pair_width = pair_grid.shape[2]
    samples = sample_index.shape[0]
    align_width = alignment_pool.shape[2]
    head_count = pair_logit.shape[1]
    head_total = average_proj.shape[1] // 2
    head_dim = head_total // head_count
    quarter = samples // n_col
    sample_start = lax.axis_index("col") * quarter

    norm_t, norm_flat = drawn_alignments(alignment_pool, sample_index)
    turned = along_rows(norm_flat)

    mix_t, pack = made_ready(norm_t, outer_proj, outer_mix, triangle_proj, 16)
    turned, mix_t, pack = lax.optimization_barrier((turned, mix_t, pack))
    parts, other, place, codes = gathered_pieces(turned)
    row_start = lax.axis_index(ROW) * tok_row
    scalars = [
        value.astype(jnp.int32).reshape(1) for value in (place, row_start, lax.axis_index("col"))
    ]
    pair_one, pair_norm, weights, factors = pair_part(
        scalars + [token_mask], codes, parts, other, pack, mix_t, samples, pair_grid,
        pair_logit.T, token_mask.reshape(n_col, tok_col),
    )

    factors, parts, other, pool, index = lax.optimization_barrier(
        (factors, parts, other, alignment_pool, sample_index)
    )
    received = lax.all_to_all(factors, ROW_COL, split_axis=0, concat_axis=0, tiled=True)

    value_weight = average_proj[:, :head_total].reshape(align_width, head_count, head_dim)
    gate_weight = average_proj[:, head_total:]
    partial_total = jnp.sum(weights, axis=2)
    low_weights = weights.astype(bf16).reshape(tok_row * head_count, tok_col)
    half = tok_col // 2
    drawn = 0.0
    for n, pieces in enumerate((parts, other)):
        row = lax.broadcasted_iota(jnp.int32, (tok_col, half), 0)
        lane = lax.broadcasted_iota(jnp.int32, (tok_col, half), 1)
        code = jnp.repeat(jnp.array(codes[n * len(codes) // 2 :][: half // tok_row]), tok_row)
        source = (place ^ code[None, :]) * tok_row + lane % tok_row
        pick = jnp.where(row == source, 1.0, 0.0).astype(bf16)
        sorted_weights = jnp.dot(low_weights, pick, preferred_element_type=f32).astype(bf16)
        drawn = drawn + jnp.dot(
            sorted_weights, pieces.reshape(half, samples * align_width),
            preferred_element_type=f32,
        )
    drawn = drawn.astype(bf16).reshape(tok_row, head_count, samples, align_width)
    partial_sum = jnp.einsum(
        "ihsm,mhc->sihc", drawn, value_weight, preferred_element_type=f32
    ).astype(bf16).reshape(n_col, quarter, tok_row, head_total)
    high = partial_total.astype(bf16)
    low = (partial_total - high.astype(f32)).astype(bf16)
    total_row = jnp.concatenate([high, low], axis=1)
    total_row = jnp.pad(total_row, ((0, 0), (0, head_total - 2 * head_count)))
    total_row = jnp.broadcast_to(total_row, (n_col, 1, tok_row, head_total))
    sums = jnp.concatenate([partial_sum, total_row], axis=1)
    sums = scattered_sum(sums, "col")
    received, sums = lax.optimization_barrier((received, sums))
    totals = sums[quarter, :, :head_count] + sums[quarter, :, head_count : 2 * head_count]
    weighted = sums[:quarter]
    own_index = lax.dynamic_slice_in_dim(index, sample_start, quarter, 0)
    own_align = jnp.take(pool, own_index, axis=0, mode="clip")
    own_norm = normalize(own_align, 2).astype(bf16)
    gate_values = jax.nn.sigmoid(
        jnp.einsum("sim,mk->sik", own_norm, gate_weight, preferred_element_type=f32)
    )
    share = jnp.repeat(1.0 / totals, head_dim, axis=1)
    averaged = (gate_values * weighted * share).astype(bf16)
    align_update = jnp.einsum("sik,km->sim", averaged, average_mix, preferred_element_type=f32)
    own_next = (own_align.astype(f32) + align_update).astype(bf16)
    alignment_next = lax.all_gather(own_next, "col", axis=0, tiled=True)

    result = triangle(received.reshape(n_row, n_col, 2, tok_row, tok_col))
    product = lax.all_to_all(
        result.reshape(n_row * n_col, tok_row, tok_col), ROW_COL,
        split_axis=0, concat_axis=0, tiled=True,
    )
    flat_norm = pair_norm.reshape(tok_row * tok_col, pair_width)
    gate_out = jax.nn.sigmoid(
        jnp.dot(flat_norm, triangle_proj[:, 4 * pair_width :], preferred_element_type=f32)
    ).reshape(pair_grid.shape)
    return tuple(
        tail(
            product, pair_one, gate_out, triangle_mix, transition_up, transition_down,
            alignment_next,
        )
    )


def solution(mesh):
    n_groups, n_row, n_col = mesh.shape["groups"], mesh.shape["row"], mesh.shape["col"]
    split = Mesh(
        mesh.devices.reshape(n_groups, n_col, n_row // n_col // 2, 2, n_col),
        ("groups", "part", "near", "core", "col"),
    )
    placed = (
        P(GROUPS_ROW, "col", None),
        P("groups", ROW, None),
        P("groups"),
        P("groups"),
    ) + (P(),) * 9
    return jax.shard_map(
        on_device,
        mesh=split,
        in_specs=placed,
        out_specs=(P(GROUPS_ROW, "col", None), P("groups", ROW, None)),
        check_vma=False,
    )
```
